256 devices in a mesh: seq: 16 (over y, x), grp: 16 (over z, core).
Axes of the slice: x: 4, y: 4, z: 8, core: 2. Of those that a mesh axis runs over, the one named last changes fastest.
Arguments:
- conv_input: bfloat16 [16, 8192, 5120], P('grp', 'seq'), may hold values from -6 to 6
- step_raw: float32 [16, 64, 8192], P('grp', None, 'seq'), may hold values from -5 to 0
- decay_rate: float32 [64], replicated, may hold values from 0 to 2, as said below
- conv_weight: bfloat16 [4, 5120], replicated, may hold values from -3 to 3
- conv_bias: bfloat16 [5120], replicated, may hold values from -3 to 3
- norm_gain: float32 [4096], replicated, may hold values from 0.5 to 1.5
- owner_slot: int32 [16], replicated, may hold values from 0 to 15, each once
Outputs:
- mixed: bfloat16 [16, 8192, 4096], P('grp', 'seq')
- final_ssm: float32 [16, 64, 64, 128], P('seq', 'grp')
- final_conv: bfloat16 [16, 5120, 4], P('seq', 'grp')
The draws below stay inside these ranges and needn't reach their ends.
Inputs may be any that keep to these rules, and one draw needn't show every extreme that they name: `decay_rate`: positive. `owner_slot`: every decode row receives exactly one prompt.
All inputs are finite; a program needn't handle non-finite values.
Results may differ from the reference program's by a relative error of at most 0.009.
Values may be sent and summed in bfloat16 or wider, within the bound.
No kernel may reach another device: no remote copies, remote signals or barrier semaphores. Data moves between devices by JAX's collectives and lax.ppermute only.
A program may use at most 128 MiB of HBM per device.

```python
import math
import jax
import jax.numpy as jnp
from jax import lax

HEADS = 64
HEAD_DIM = 64
STATE = 128
GROUPS = 4
CONV_K = 4
BLOCK = 256
L_DEV = 512
D_IN = 4096
CH = 5120
LENGTH = 8192
PROMPTS = 16


def draw_step_raw(key, part):
    noise_key = jax.random.fold_in(key, 11)
    offset_key = jax.random.fold_in(key, 12)
    segments = LENGTH // L_DEV
    noise = 0.5 * jax.random.truncated_normal(noise_key, -3.0, 3.0, (PROMPTS, HEADS, LENGTH), jnp.float32)
    offset = jax.random.uniform(offset_key, (PROMPTS, 1, segments, 1), jnp.float32, -3.5, -2.0)
    offset = jnp.broadcast_to(offset, (PROMPTS, 1, segments, L_DEV)).reshape(PROMPTS, 1, LENGTH)
    return noise + offset


def draw_decay_rate(key, part):
    pick_key = jax.random.fold_in(key, 21)
    fast_key = jax.random.fold_in(key, 22)
    slow_key = jax.random.fold_in(key, 23)
    share = 0.5
    quick = jax.random.uniform(pick_key, (HEADS,), jnp.float32) < share
    fast_rate = jnp.exp(jax.random.uniform(fast_key, (HEADS,), jnp.float32, math.log(0.5), math.log(2.0)))
    slow_rate = jnp.exp(jax.random.uniform(slow_key, (HEADS,), jnp.float32, math.log(2.0 / LENGTH), math.log(15.0 / LENGTH)))
    return jnp.where(quick, fast_rate, slow_rate)


def block_levels(own_key, dims, shards, least, high):
    level, own = 1.0, jax.random.fold_in(own_key, 6)
    for position, blocks in shards:
        heights = jnp.exp(jax.random.uniform(jax.random.fold_in(own, position), (blocks,), jnp.float32, least / len(shards), high / len(shards)))
        level = level * jnp.repeat(heights, dims[position] // blocks).reshape([-1 if axis == position else 1 for axis in range(len(dims))])
    return level


def scatter_about(own_key, shape, scale, limit, cuts=(), kind=jnp.bfloat16):
    drawn = scale * jax.random.normal(own_key, shape, jnp.float32)
    if cuts:
        drawn = drawn * block_levels(own_key, shape, cuts, -0.22, 0.18)
    return jnp.clip(drawn, -limit, limit).astype(kind)


def setup_inputs(seed: int = 0) -> dict:
    streams_of = jax.random.split(jax.random.key(seed), 8)
    conv_input = scatter_about(streams_of[0], (PROMPTS, LENGTH, CH), 1.0, 6.0, ((0, 16), (1, 16)))
    step_raw = draw_step_raw(jax.random.fold_in(streams_of[7], 71), 0)
    decay_rate = draw_decay_rate(jax.random.fold_in(streams_of[7], 71), 0)
    conv_weight = scatter_about(streams_of[3], (CONV_K, CH), CONV_K ** -0.5, 3.0)
    conv_bias = scatter_about(streams_of[4], (CH,), 0.5, 3.0)
    norm_gain = jnp.clip(1.0 + 0.1 * jax.random.normal(streams_of[5], (D_IN,), jnp.float32), 0.5, 1.5)
    owner_slot = jax.random.permutation(streams_of[6], PROMPTS).astype(jnp.int32)
    return dict(conv_input=conv_input, step_raw=step_raw, decay_rate=decay_rate, conv_weight=conv_weight, conv_bias=conv_bias, norm_gain=norm_gain, owner_slot=owner_slot)


NORM_EPS = 1.0

def conv_silu(padded, conv_weight, conv_bias):
    width = conv_weight.shape[0]
    length = padded.shape[0] - width + 1
    total = jnp.zeros((length, padded.shape[1]), jnp.float32) + conv_bias.astype(jnp.float32)[None, :]
    for offset in range(width):
        total = total + conv_weight[offset].astype(jnp.float32)[None, :] * padded[offset:offset + length].astype(jnp.float32)
    return jax.nn.silu(total).astype(jnp.bfloat16)

def rounded(value):
    return lax.optimization_barrier(value.astype(jnp.bfloat16)).astype(jnp.float32)

def block_terms(inputs, b_matrix, c_matrix, step_size, log_decay):
    width = log_decay.shape[-1]
    summed = jnp.cumsum(log_decay, axis=-1)
    scores = jnp.einsum('tgn,ugn->gtu', c_matrix.astype(jnp.float32), b_matrix.astype(jnp.float32))
    causal = jnp.arange(width)[:, None] >= jnp.arange(width)[None, :]
    spread = jnp.exp(jnp.minimum(summed[:, :, :, None] - summed[:, :, None, :], 0.0))
    weights = jnp.where(causal, spread, 0.0) * step_size[:, :, None, :] * scores[:, None, :, :]
    intra = jnp.einsum('gktu,ugkp->tgkp', rounded(weights), inputs.astype(jnp.float32))
    tail = jnp.exp(summed[:, :, -1:] - summed) * step_size
    scaled = tail[..., None] * jnp.swapaxes(b_matrix, 0, 1).astype(jnp.float32)[:, None, :, :]
    local = jnp.einsum('gkun,ugkp->gkpn', rounded(scaled), inputs.astype(jnp.float32))
    return (intra, local, jnp.exp(summed[:, :, -1]), jnp.exp(summed))

def from_state(c_matrix, carried, scale):
    reach = jnp.einsum('tgn,gkpn->tgkp', c_matrix.astype(jnp.float32), rounded(carried))
    return reach * jnp.transpose(scale, (2, 0, 1))[..., None]

def one_prompt(conv_rows, raw_steps, decay_rate, conv_weight, conv_bias, norm_gain):
    width = conv_weight.shape[0]
    padded = jnp.concatenate([jnp.zeros((width - 1, conv_rows.shape[1]), conv_rows.dtype), conv_rows], axis=0)
    conved = conv_silu(padded, conv_weight, conv_bias)
    blocks = LENGTH // BLOCK
    per_group = HEADS // GROUPS
    inputs = conved[:, :D_IN].reshape(blocks, BLOCK, GROUPS, per_group, HEAD_DIM)
    b_matrix = conved[:, D_IN:D_IN + GROUPS * STATE].reshape(blocks, BLOCK, GROUPS, STATE)
    c_matrix = conved[:, D_IN + GROUPS * STATE:].reshape(blocks, BLOCK, GROUPS, STATE)
    step_size = jax.nn.softplus(raw_steps)
    log_decay = -step_size * decay_rate[:, None]
    step_size = jnp.moveaxis(step_size.reshape(GROUPS, per_group, blocks, BLOCK), 2, 0)
    log_decay = jnp.moveaxis(log_decay.reshape(GROUPS, per_group, blocks, BLOCK), 2, 0)

    def advance(carried, pieces):
        intra, local, decay, scale = block_terms(pieces[0], pieces[1], pieces[2], pieces[3], pieces[4])
        output = intra + from_state(pieces[2], carried, scale)
        return (decay[:, :, None, None] * carried + local, output)
    start = jnp.zeros((GROUPS, per_group, HEAD_DIM, STATE), jnp.float32)
    final, outputs = lax.scan(advance, start, (inputs, b_matrix, c_matrix, step_size, log_decay))
    values = outputs.reshape(LENGTH, GROUPS, per_group * HEAD_DIM)
    norm_scale = lax.rsqrt(lax.optimization_barrier(jnp.mean(values * values, axis=-1)) + NORM_EPS)
    mixed = ((values * norm_scale[..., None]).reshape(LENGTH, D_IN) * norm_gain[None, :]).astype(jnp.bfloat16)
    kept = jnp.transpose(conv_rows[LENGTH - width:], (1, 0))
    return (mixed, final.reshape(HEADS, HEAD_DIM, STATE), kept)

def reference(conv_input, step_raw, decay_rate, conv_weight, conv_bias, norm_gain, owner_slot):

    def run(pieces):
        return one_prompt(pieces[0], pieces[1], decay_rate, conv_weight, conv_bias, norm_gain)
    mixed, final_state, kept = lax.map(run, (conv_input, step_raw))
    final_ssm = jnp.zeros_like(final_state).at[owner_slot].set(final_state)
    final_conv = jnp.zeros_like(kept).at[owner_slot].set(kept)
    return (mixed, final_ssm, final_conv)
```

```python
import functools
import math

import jax
import jax.numpy as jnp
from jax import lax
from jax.experimental import pallas as pl
from jax.experimental.pallas import tpu as pltpu
from jax.sharding import PartitionSpec as P

HEADS = 64
HEAD_DIM = 64
STATE = 128
GROUPS = 4
PER_GROUP = HEADS // GROUPS
GROUP_CH = PER_GROUP * HEAD_DIM
BLOCK = 256
D_IN = 4096
CH = 5120
L_DEV = 512
SHARDS = 16
OWN_CH = 256
SENT_ROWS = 136
PIECES = 2
PIECE_ROWS = 72
VMEM_LIMIT = 67043328
NORM_EPS = 1.0
LOG2E = math.log2(math.e)
CAP = 64.0

F32 = jnp.float32
BF16 = jnp.bfloat16


def dot(a, b):
    return lax.dot_general(a, b, (((1,), (0,)), ((), ())), preferred_element_type=F32)


def three_pieces(v):
    hi = v.astype(BF16).astype(F32)
    rest = v - hi
    mid = rest.astype(BF16).astype(F32)
    return hi, mid, (rest - mid).astype(BF16).astype(F32)


TAIL, GROWN = 0, 48


def spread_matrix(first):
    row = lax.broadcasted_iota(jnp.int32, (128, GROUP_CH), 0)
    col = lax.broadcasted_iota(jnp.int32, (128, GROUP_CH), 1)
    hit = (row >= first) & (row < first + 48) & (row % PER_GROUP == col // HEAD_DIM)
    return jnp.where(hit, 1.0, 0.0).astype(BF16)


def prep_kernel(step_ref, rate_ref, row_ref, sum_ref, col_ref):
    dt = jax.nn.softplus(step_ref[0])
    near = lax.broadcasted_iota(jnp.int32, (HEADS, HEADS), 0)
    far = lax.broadcasted_iota(jnp.int32, (HEADS, HEADS), 1)
    decay = jnp.sum(jnp.where(near == far, rate_ref[...], 0.0), axis=1, keepdims=True)
    rate = dt * (decay * -LOG2E)
    later = lax.broadcasted_iota(jnp.int32, (BLOCK, BLOCK), 0)
    earlier = lax.broadcasted_iota(jnp.int32, (BLOCK, BLOCK), 1)
    upto = jnp.where(later <= earlier, 1.0, 0.0).astype(BF16)
    zero = jnp.zeros((2 * PER_GROUP, BLOCK), F32)
    for j in range(L_DEV // BLOCK):
        span = slice(j * BLOCK, (j + 1) * BLOCK)
        dt_j = dt[:, span]
        stacked = jnp.concatenate(three_pieces(rate[:, span]), axis=0).astype(BF16)
        sums = dot(stacked, upto)
        cs = sums[:HEADS] + sums[HEADS : 2 * HEADS] + sums[2 * HEADS :]
        row_ref[:, span] = cs - jnp.log2(dt_j)
        tail = three_pieces(jnp.exp2(cs[:, BLOCK - 1 :] - cs) * dt_j)
        grown = three_pieces(jnp.exp2(cs))
        turned = jnp.transpose(jnp.concatenate([cs, cs], axis=0))
        for g in range(GROUPS):
            heads = slice(g * PER_GROUP, (g + 1) * PER_GROUP)
            parts = [v[heads] for v in tail + grown] + [zero]
            col_ref[g, span, :] = jnp.transpose(jnp.concatenate(parts, axis=0)).astype(BF16)
            sum_ref[g, span, :] = turned if g == 0 else pltpu.roll(turned, 128 - g * PER_GROUP, 1)


def prep(step_raw, decay_rate):
    return pl.pallas_call(
        prep_kernel,
        out_shape=(
            jax.ShapeDtypeStruct((HEADS, L_DEV), F32),
            jax.ShapeDtypeStruct((GROUPS, L_DEV, 128), F32),
            jax.ShapeDtypeStruct((GROUPS, L_DEV, 128), BF16),
        ),
        cost_estimate=pl.CostEstimate(flops=10**9, bytes_accessed=2**21, transcendentals=0),
        compiler_params=pltpu.CompilerParams(vmem_limit_bytes=VMEM_LIMIT),
        name="prep",
    )(step_raw, decay_rate)


CONV_ROWS = 32
CONV_AT = (0, 256, 640, 896)


def conv_kernel(
    prompt_ref, x_ref, b_ref, c_ref, hx_ref, hb_ref, hc_ref, wx_ref, wb_ref, wc_ref, bx_ref, bb_ref,
    bc_ref, last_ref, col_ref, xo_ref, bo_ref, co_ref, e0_ref, p_ref, xf, xs, spread, regrown,
):
    within = prompt_ref[0] % 4

    @pl.when(pl.program_id(0) == 0)
    def _():
        spread[...] = spread_matrix(TAIL)
        regrown[...] = spread_matrix(GROWN)


    def load(slot, ref, halo_ref, lanes):
        xf[slot, 5:8, :] = halo_ref[0, :, lanes].astype(F32)
        xf[slot, 8 : 8 + L_DEV, :] = ref[0, :, lanes].astype(F32)

    for k in range(8):
        load(k, x_ref, hx_ref, slice(k * 128, (k + 1) * 128))
    load(8, b_ref, hb_ref, slice(0, 128))
    load(9, c_ref, hc_ref, slice(0, 128))

    def taps(w_ref, bias_ref, lanes):
        w = w_ref[:, lanes].astype(F32) * 0.5
        return [w[k : k + 1] for k in range(4)], bias_ref[:, lanes].astype(F32) * 0.5

    def conved(slot, r0, w, bias):
        half = bias + w[0] * xf[slot, 5 + r0 : 5 + r0 + CONV_ROWS, :]
        for k in range(1, 4):
            half = half + w[k] * xf[slot, 5 + k + r0 : 5 + k + r0 + CONV_ROWS, :]
        return (half + half * jnp.tanh(half)).astype(BF16)

    for slot, w_ref, bias_ref, out in ((8, wb_ref, bb_ref, bo_ref), (9, wc_ref, bc_ref, co_ref)):
        w, bias = taps(w_ref, bias_ref, slice(0, 128))
        for r0 in range(0, L_DEV, CONV_ROWS):
            out[r0 : r0 + CONV_ROWS, :] = conved(slot, r0, w, bias)

    for pair in range(4):
        both = [taps(wx_ref, bx_ref, slice(k * 128, (k + 1) * 128)) for k in (2 * pair, 2 * pair + 1)]
        lanes2 = slice(pair * 256, (pair + 1) * 256)
        for r0 in range(0, L_DEV, CONV_ROWS):
            rows = slice(r0, r0 + CONV_ROWS)
            tail = dot(col_ref[0, rows, :], spread[:, lanes2])
            for half in range(2):
                k = 2 * pair + half
                lanes = slice(k * 128, (k + 1) * 128)
                value = conved(k, r0, *both[half])
                xo_ref[rows, lanes] = value
                xs[rows, lanes] = (value.astype(F32) * tail[:, half * 128 : half * 128 + 128]).astype(BF16)

    ends = jnp.concatenate([col_ref[0, 240:256, :], col_ref[0, 496:512, :]], axis=0)
    decays = dot(ends, regrown[...])
    first, second = decays[15:16], decays[31:32]
    last = last_ref[0].astype(F32)[12:16]
    bt = [
        jnp.transpose(bo_ref[j * BLOCK : (j + 1) * BLOCK, :].astype(F32)).astype(BF16) for j in range(2)
    ]
    for s in range(4):
        lanes = slice(s * OWN_CH, (s + 1) * OWN_CH)
        slot = s ^ within
        e0 = dot(bt[0], xs[:BLOCK, lanes])
        e1 = dot(bt[1], xs[BLOCK:, lanes])
        e0_ref[0, :, lanes] = e0.astype(BF16)
        p_ref[slot, :STATE, :] = (second[:, lanes] * e0 + e1).astype(BF16)
        hi, mid, _ = three_pieces(first[:, lanes] * second[:, lanes])
        at = CONV_AT[s]
        ends = [last[k : k + 1, at + 256 : at + 384] for k in range(4)]
        extra = [
            hi, mid, last[:, at : at + 256],
            jnp.concatenate(ends[:2], axis=1), jnp.concatenate(ends[2:], axis=1),
        ]
        p_ref[slot, STATE:, :] = jnp.concatenate(extra, axis=0).astype(BF16)


def conv(rows, before, weight, bias, cols, prompt):
    def at(height, width, first):
        return pl.BlockSpec((1, height, width), lambda g, p: (0, 0, first + g))

    def flat(height, width, first):
        return pl.BlockSpec((height, width), lambda g, p: (0, first + g))

    return pl.pallas_call(
        conv_kernel,
        grid_spec=pltpu.PrefetchScalarGridSpec(
            num_scalar_prefetch=1,
            grid=(GROUPS,),
            in_specs=[
                at(L_DEV, GROUP_CH, 0), at(L_DEV, 128, 32), at(L_DEV, 128, 36),
                at(3, GROUP_CH, 0), at(3, 128, 32), at(3, 128, 36),
                flat(4, GROUP_CH, 0), flat(4, 128, 32), flat(4, 128, 36),
                flat(1, GROUP_CH, 0), flat(1, 128, 32), flat(1, 128, 36),
                pl.BlockSpec((1, 16, CH // GROUPS), lambda g, p: (0, L_DEV // 16 - 1, g)),
                pl.BlockSpec((1, L_DEV, 128), lambda g, p: (g, 0, 0)),
            ],
            out_specs=(
                flat(L_DEV, GROUP_CH, 0),
                flat(L_DEV, 128, 0),
                flat(L_DEV, 128, 0),
                pl.BlockSpec((1, STATE, GROUP_CH), lambda g, p: (g, 0, 0)),
                pl.BlockSpec((4, SENT_ROWS, OWN_CH), lambda g, p: (g ^ (p[0] // 4), 0, 0)),
            ),
            scratch_shapes=[
                pltpu.VMEM((10, L_DEV + 8, 128), F32),
                pltpu.VMEM((L_DEV, GROUP_CH), BF16),
                pltpu.VMEM((128, GROUP_CH), BF16),
                pltpu.VMEM((128, GROUP_CH), BF16),
            ],
        ),
        out_shape=(
            jax.ShapeDtypeStruct((L_DEV, D_IN), BF16),
            jax.ShapeDtypeStruct((L_DEV, GROUPS * STATE), BF16),
            jax.ShapeDtypeStruct((L_DEV, GROUPS * STATE), BF16),
            jax.ShapeDtypeStruct((GROUPS, STATE, GROUP_CH), BF16),
            jax.ShapeDtypeStruct((SHARDS, SENT_ROWS, OWN_CH), BF16),
        ),
        cost_estimate=pl.CostEstimate(flops=10 * 10**9, bytes_accessed=14 * 2**20, transcendentals=0),
        compiler_params=pltpu.CompilerParams(vmem_limit_bytes=VMEM_LIMIT),
        name="conv_state",
    )(prompt, rows, rows, rows, before, before, before, weight, weight, weight, bias, bias, bias, rows, cols)


def intra_kernel(x_ref, b_ref, c_ref, row_ref, col_ref, y_ref):
    half = BLOCK // 2
    scores = lax.dot_general(
        c_ref[...], b_ref[...], (((1,), (1,)), ((), ())), preferred_element_type=F32
    )
    t = lax.broadcasted_iota(jnp.int32, (half, half), 0)
    u = lax.broadcasted_iota(jnp.int32, (half, half), 1)
    s00 = jnp.where(u <= t, scores[:half, :half], 0.0)
    s10 = scores[half:, :half]
    s11 = jnp.where(u <= t, scores[half:, half:], 0.0)
    low = lax.broadcasted_iota(jnp.int32, (BLOCK, 128), 1) < HEAD_DIM
    for pair in range(PER_GROUP // 2):
        lanes = slice(pair * 128, (pair + 1) * 128)
        x = x_ref[:, lanes]
        zero = jnp.zeros_like(x)
        xl, xh = jnp.where(low, x, zero), jnp.where(low, zero, x)
        top, bottom = [], []
        for h in (2 * pair, 2 * pair + 1):
            cs0 = jnp.broadcast_to(col_ref[0, :half, h : h + 1], (half, half))
            cs1 = jnp.broadcast_to(col_ref[0, half:, h : h + 1], (half, half))
            a0 = row_ref[h : h + 1, :half]
            a1 = row_ref[h : h + 1, half:]
            top.append((jnp.exp2(jnp.minimum(cs0 - a0, CAP)) * s00).astype(BF16))
            bottom.append((jnp.exp2(cs1 - a0) * s10).astype(BF16))
            bottom.append((jnp.exp2(jnp.minimum(cs1 - a1, CAP)) * s11).astype(BF16))
        above = dot(jnp.concatenate(top, axis=1), jnp.concatenate([xl[:half], xh[:half]], axis=0))
        below = dot(jnp.concatenate(bottom, axis=1), jnp.concatenate([xl, xh], axis=0))
        y_ref[:half, lanes] = above.astype(BF16)
        y_ref[half:, lanes] = below.astype(BF16)


def intra(x, b, c, sums, cols, groups, first):
    return pl.pallas_call(
        intra_kernel,
        grid=(groups, L_DEV // BLOCK),
        in_specs=[
            pl.BlockSpec((BLOCK, GROUP_CH), lambda g, j: (j, first + g)),
            pl.BlockSpec((BLOCK, 128), lambda g, j: (j, first + g)),
            pl.BlockSpec((BLOCK, 128), lambda g, j: (j, first + g)),
            pl.BlockSpec((PER_GROUP, BLOCK), lambda g, j: (first + g, j)),
            pl.BlockSpec((1, BLOCK, 128), lambda g, j: (first + g, j, 0)),
        ],
        out_specs=pl.BlockSpec((BLOCK, GROUP_CH), lambda g, j: (j, g)),
        out_shape=jax.ShapeDtypeStruct((L_DEV, groups * GROUP_CH), BF16),
        cost_estimate=pl.CostEstimate(
            flops=groups * 3 * 10**9, bytes_accessed=groups * 3 * 2**20, transcendentals=0
        ),
        compiler_params=pltpu.CompilerParams(vmem_limit_bytes=VMEM_LIMIT),
        name="intra",
    )(x, b, c, sums, cols)


def scan_kernel(r_ref, p_ref, *piece_refs):
    state = jnp.zeros((STATE, OWN_CH), F32)
    for d in range(SHARDS):
        p_ref[d] = state.astype(BF16)
        extra = r_ref[d, STATE:, :].astype(F32)
        state = (extra[0:1] + extra[1:2]) * state + r_ref[d, :STATE, :].astype(F32)
    size = STATE // PIECES
    zero = jnp.zeros((PIECE_ROWS - size - 3, OWN_CH), F32)
    for k, ref in enumerate(piece_refs):
        rows = extra[2 + 2 * k : 4 + 2 * k]
        parts = [state[k * size : k * size + size], rows, extra[6 + k : 7 + k], zero]
        ref[...] = jnp.concatenate(parts, axis=0).astype(BF16)


def scan(got):
    piece = jax.ShapeDtypeStruct((PIECE_ROWS, OWN_CH), BF16)
    out = pl.pallas_call(
        scan_kernel,
        out_shape=[jax.ShapeDtypeStruct((SHARDS, STATE, OWN_CH), BF16)] + [piece] * PIECES,
        cost_estimate=pl.CostEstimate(flops=10**9, bytes_accessed=2**22, transcendentals=0),
        compiler_params=pltpu.CompilerParams(vmem_limit_bytes=VMEM_LIMIT),
        name="scan",
    )(got)
    return out[0], out[1:]


def pack_kernel(place_ref, prompt_ref, owner_ref, *refs):
    pieces, p_ref = refs[:-1], refs[-1]
    p_ref[...] = jnp.zeros_like(p_ref)
    for k in range(PIECES):
        p_ref[owner_ref[place_ref[0] ^ prompt_ref[0] ^ k]] = pieces[k][...]


SMEM = pl.BlockSpec(memory_space=pltpu.SMEM)
VMEM = pl.BlockSpec(memory_space=pltpu.VMEM)


def pack(place, prompt, owner_slot, pieces):
    return pl.pallas_call(
        pack_kernel,
        in_specs=[SMEM] * 3 + [VMEM] * PIECES,
        out_shape=jax.ShapeDtypeStruct((SHARDS, PIECE_ROWS, OWN_CH), BF16),
        cost_estimate=pl.CostEstimate(flops=10**8, bytes_accessed=2**19, transcendentals=0),
        compiler_params=pltpu.CompilerParams(vmem_limit_bytes=VMEM_LIMIT),
        name="pack",
    )(place, prompt, owner_slot, *pieces)


def unpack_kernel(place_ref, prompt_ref, owner_ref, r_ref, ssm_ref, conv_ref):
    size = STATE // PIECES
    mine = 0
    for p in range(SHARDS):
        mine = jnp.where(owner_ref[p] == place_ref[0], p, mine)
    parts = [r_ref[mine ^ prompt_ref[0] ^ k].astype(F32) for k in range(PIECES)]
    state = jnp.concatenate([part[:size] for part in parts], axis=0)
    ssm_ref[...] = jnp.transpose(state)
    rows = jnp.concatenate([part[size : size + 2] for part in parts], axis=0)
    ends = [part[size + 2 : size + 3, n * 128 : n * 128 + 128] for part in parts for n in range(2)]
    window = jnp.concatenate([rows, jnp.concatenate(ends, axis=0)], axis=1)
    moved = jnp.concatenate([window[:, 64:], window[:, :64]], axis=1)
    odd = prompt_ref[0] % 2 == 1
    conv_ref[...] = jnp.where(odd, moved, window)[:, : CH // SHARDS].astype(BF16)


def unpack(place, prompt, owner_slot, got):
    return pl.pallas_call(
        unpack_kernel,
        in_specs=[SMEM] * 3 + [VMEM],
        out_shape=(
            jax.ShapeDtypeStruct((OWN_CH, STATE), F32),
            jax.ShapeDtypeStruct((4, CH // SHARDS), BF16),
        ),
        cost_estimate=pl.CostEstimate(flops=10**8, bytes_accessed=2**19, transcendentals=0),
        compiler_params=pltpu.CompilerParams(vmem_limit_bytes=VMEM_LIMIT),
        name="unpack",
    )(place, prompt, owner_slot, got)


def out_kernel(prompt_ref, y_ref, c_ref, col_ref, e0_ref, state_ref, gain_ref, o_ref, ys, spread):
    within = prompt_ref[0] % 4

    @pl.when(pl.program_id(0) == 0)
    def _():
        spread[...] = spread_matrix(GROWN)

    decay = dot(col_ref[0, 240:256, :], spread[...])[15:16]
    for j in range(2):
        rows = slice(j * BLOCK, (j + 1) * BLOCK)
        c = c_ref[rows, :]
        grown = col_ref[0, rows, :]
        total = jnp.zeros((BLOCK, 128), F32)
        for s in range(4):
            lanes = slice(s * OWN_CH, (s + 1) * OWN_CH)
            state = state_ref[s ^ within]
            if j == 1:
                state = (decay[:, lanes] * state.astype(F32) + e0_ref[0, :, lanes].astype(F32)).astype(BF16)
            y = y_ref[rows, lanes].astype(F32) + dot(grown, spread[:, lanes]) * dot(c, state)
            ys[:, lanes] = y
            total = total + y[:, :128] * y[:, :128] + y[:, 128:] * y[:, 128:]
        mean = jnp.sum(total, axis=1, keepdims=True) * (1.0 / GROUP_CH)
        scale = lax.rsqrt(mean + NORM_EPS)
        o_ref[0, rows, :] = (ys[...] * scale * gain_ref[...]).astype(BF16)


def finish(y, c, cols, e0, states, gain, prompt):
    return pl.pallas_call(
        out_kernel,
        grid_spec=pltpu.PrefetchScalarGridSpec(
            num_scalar_prefetch=1,
            grid=(GROUPS,),
            in_specs=[
                pl.BlockSpec((L_DEV, GROUP_CH), lambda g, p: (0, g)),
                pl.BlockSpec((L_DEV, 128), lambda g, p: (0, g)),
                pl.BlockSpec((1, L_DEV, 128), lambda g, p: (g, 0, 0)),
                pl.BlockSpec((1, STATE, GROUP_CH), lambda g, p: (g, 0, 0)),
                pl.BlockSpec((4, STATE, OWN_CH), lambda g, p: (g ^ (p[0] // 4), 0, 0)),
                pl.BlockSpec((1, GROUP_CH), lambda g, p: (0, g)),
            ],
            out_specs=pl.BlockSpec((1, L_DEV, GROUP_CH), lambda g, p: (0, 0, g)),
            scratch_shapes=[pltpu.VMEM((BLOCK, GROUP_CH), F32), pltpu.VMEM((128, GROUP_CH), BF16)],
        ),
        out_shape=jax.ShapeDtypeStruct((1, L_DEV, D_IN), BF16),
        cost_estimate=pl.CostEstimate(flops=8 * 10**9, bytes_accessed=12 * 2**20, transcendentals=0),
        compiler_params=pltpu.CompilerParams(vmem_limit_bytes=VMEM_LIMIT),
        name="finish",
    )(prompt, y, c, cols, e0, states, gain)


def exchange(pieces, axis):
    return lax.all_to_all(pieces, axis, split_axis=0, concat_axis=0, tiled=True)


def body(conv_input, step_raw, decay_rate, conv_weight, conv_bias, norm_gain, owner_slot):
    place = lax.axis_index("seq").astype(jnp.int32)[None]
    prompt = lax.axis_index("grp").astype(jnp.int32)[None]
    route = [(d, d + 1) for d in range(SHARDS - 1)]
    before = lax.ppermute(conv_input[:, L_DEV - 3 :, :], "seq", route)
    starts, sums, cols = prep(step_raw, decay_rate[None, :])
    x, b, c, e0, sent = conv(conv_input, before, conv_weight, conv_bias[None, :], cols, prompt)
    y = intra(x, b, c, starts, sums, GROUPS, 0)
    got, y = lax.optimization_barrier((exchange(sent, "seq"), y))
    states, final = scan(got)
    entering = exchange(states, "seq")
    pieces = []
    for k in range(PIECES):
        route = [
            (r * SHARDS + p, (r ^ k) * SHARDS + (r ^ p)) for r in range(SHARDS) for p in range(SHARDS)
        ]
        pieces.append(lax.ppermute(final[k], ("seq", "grp"), route))
    packed = pack(place, prompt, owner_slot, pieces)
    entering, packed = lax.optimization_barrier((entering, packed))
    arrived = exchange(packed, "seq")
    mixed = finish(y, c, cols, e0, entering, norm_gain[None, :], prompt)
    ssm, rows = unpack(place, prompt, owner_slot, arrived)
    return mixed, ssm.reshape(1, 4, HEAD_DIM, STATE), jnp.transpose(rows)[None]


def solution(mesh):
    return jax.shard_map(
        body,
        mesh=mesh,
        in_specs=(P("grp", "seq", None), P("grp", None, "seq"), P(), P(), P(), P(), P()),
        out_specs=(P("grp", "seq", None), P("seq", "grp", None, None), P("seq", "grp", None)),
        check_vma=False,
    )
```

```python
import functools
import math

import jax
import jax.numpy as jnp
from jax import lax
from jax.experimental import pallas as pl
from jax.experimental.pallas import tpu as pltpu
from jax.sharding import PartitionSpec as P

HEADS = 64
HEAD_DIM = 64
STATE = 128
GROUPS = 4
PER_GROUP = HEADS // GROUPS
GROUP_CH = PER_GROUP * HEAD_DIM
BLOCK = 256
D_IN = 4096
CH = 5120
L_DEV = 512
SHARDS = 16
OWN_CH = 256
SENT_ROWS = 136
PIECES = 2
FLIP = SHARDS - 1
PIECE_ROWS = 72
VMEM_LIMIT = 67043328
NORM_EPS = 1.0
LOG2E = math.log2(math.e)
CAP = 64.0

SMEM = pl.BlockSpec(memory_space=pltpu.SMEM)
VMEM = pl.BlockSpec(memory_space=pltpu.VMEM)
ANY = pl.BlockSpec(memory_space=pl.ANY)

F32 = jnp.float32
BF16 = jnp.bfloat16


def dot(a, b):
    return lax.dot_general(a, b, (((1,), (0,)), ((), ())), preferred_element_type=F32)


def three_pieces(v):
    hi = v.astype(BF16).astype(F32)
    rest = v - hi
    mid = rest.astype(BF16).astype(F32)
    return hi, mid, (rest - mid).astype(BF16).astype(F32)


TAIL, GROWN = 0, 48


def spread_matrix(first):
    row = lax.broadcasted_iota(jnp.int32, (128, GROUP_CH), 0)
    col = lax.broadcasted_iota(jnp.int32, (128, GROUP_CH), 1)
    hit = (row >= first) & (row < first + 48) & (row % PER_GROUP == col // HEAD_DIM)
    return jnp.where(hit, 1.0, 0.0).astype(BF16)


def prep_kernel(step_ref, rate_ref, row_ref, sum_ref, col_ref):
    dt = jax.nn.softplus(step_ref[0])
    near = lax.broadcasted_iota(jnp.int32, (HEADS, HEADS), 0)
    far = lax.broadcasted_iota(jnp.int32, (HEADS, HEADS), 1)
    decay = jnp.sum(jnp.where(near == far, rate_ref[...], 0.0), axis=1, keepdims=True)
    rate = dt * (decay * -LOG2E)
    later = lax.broadcasted_iota(jnp.int32, (BLOCK, BLOCK), 0)
    earlier = lax.broadcasted_iota(jnp.int32, (BLOCK, BLOCK), 1)
    upto = jnp.where(later <= earlier, 1.0, 0.0).astype(BF16)
    zero = jnp.zeros((2 * PER_GROUP, BLOCK), F32)
    for j in range(L_DEV // BLOCK):
        span = slice(j * BLOCK, (j + 1) * BLOCK)
        dt_j = dt[:, span]
        stacked = jnp.concatenate(three_pieces(rate[:, span]), axis=0).astype(BF16)
        sums = dot(stacked, upto)
        cs = sums[:HEADS] + sums[HEADS : 2 * HEADS] + sums[2 * HEADS :]
        row_ref[:, span] = cs - jnp.log2(dt_j)
        tail = three_pieces(jnp.exp2(cs[:, BLOCK - 1 :] - cs) * dt_j)
        grown = three_pieces(jnp.exp2(cs))
        sum_ref[span, :] = jnp.transpose(jnp.concatenate([cs, cs], axis=0))
        for g in range(GROUPS):
            heads = slice(g * PER_GROUP, (g + 1) * PER_GROUP)
            parts = [v[heads] for v in tail + grown] + [zero]
            col_ref[g, span, :] = jnp.transpose(jnp.concatenate(parts, axis=0)).astype(BF16)


def prep(step_raw, decay_rate):
    return pl.pallas_call(
        prep_kernel,
        out_shape=(
            jax.ShapeDtypeStruct((HEADS, L_DEV), F32),
            jax.ShapeDtypeStruct((L_DEV, 2 * HEADS), F32),
            jax.ShapeDtypeStruct((GROUPS, L_DEV, 128), BF16),
        ),
        cost_estimate=pl.CostEstimate(flops=10**9, bytes_accessed=2**21, transcendentals=0),
        compiler_params=pltpu.CompilerParams(vmem_limit_bytes=VMEM_LIMIT),
        name="prep",
    )(step_raw, decay_rate)


CONV_ROWS = 16


def taps(w_ref, bias_ref, lanes):
    w = w_ref[:, lanes].astype(F32) * 0.5
    return [w[k : k + 1] for k in range(4)], bias_ref[:, lanes].astype(F32) * 0.5


def silu_of(values, at, w, bias):
    half = bias + w[0] * values[at : at + CONV_ROWS, :]
    for k in range(1, 4):
        half = half + w[k] * values[at + k : at + k + CONV_ROWS, :]
    return half + half * jnp.tanh(half)


def conv_kernel(
    mask_ref, x_ref, b_ref, hx_ref, hb_ref, wx_ref, wb_ref, bx_ref, bb_ref, last_ref, col_ref,
    xo_ref, bo_ref, e0_ref, p_ref, xf, xs, tails, spread, regrown,
):
    within = mask_ref[0] % 4

    @pl.when(pl.program_id(0) == 0)
    def _():
        spread[...] = spread_matrix(TAIL)
        regrown[...] = spread_matrix(GROWN)

    def load(slot, ref, halo_ref, lanes):
        xf[slot, 5:8, :] = halo_ref[0, :, lanes].astype(F32)
        xf[slot, 8 : 8 + L_DEV, :] = ref[0, :, lanes].astype(F32)

    load(8, b_ref, hb_ref, slice(0, 128))
    w, bias = taps(wb_ref, bb_ref, slice(0, 128))
    for r0 in range(0, L_DEV, CONV_ROWS):
        bo_ref[r0 : r0 + CONV_ROWS, :] = silu_of(xf.at[8], 5 + r0, w, bias).astype(BF16)
    bt = [
        jnp.transpose(bo_ref[j * BLOCK : (j + 1) * BLOCK, :].astype(F32)).astype(BF16) for j in range(2)
    ]
    ends = jnp.concatenate([col_ref[0, 240:256, :], col_ref[0, 496:512, :]], axis=0)
    decays = dot(ends, regrown[...])
    last = last_ref[0].astype(F32)[12:16]
    for s in range(4):
        wide = slice(s * OWN_CH, (s + 1) * OWN_CH)
        tails[s] = dot(col_ref[0], spread[:, wide])
        pair = (2 * s, 2 * s + 1)
        both = []
        for k in pair:
            lanes = slice(k * 128, (k + 1) * 128)
            load(k, x_ref, hx_ref, lanes)
            both.append(taps(wx_ref, bx_ref, lanes))
        for r0 in range(0, L_DEV, CONV_ROWS):
            rows = slice(r0, r0 + CONV_ROWS)
            parts = [silu_of(xf.at[k], 5 + r0, *tap) for k, tap in zip(pair, both)]
            value = jnp.concatenate(parts, axis=1)
            xo_ref[rows, wide] = value.astype(BF16)
            xs[rows, wide] = (value * tails[s, rows, :]).astype(BF16)
        first, second = decays[15:16, wide], decays[31:32, wide]
        e0 = dot(bt[0], xs[:BLOCK, wide])
        e1 = dot(bt[1], xs[BLOCK:, wide])
        e0_ref[0, :, wide] = e0.astype(BF16)
        slot = s ^ within
        p_ref[slot, :STATE, :] = (second * e0 + e1).astype(BF16)
        hi, mid, _ = three_pieces(first * second)
        at = CONV_AT[s]
        ends_of = [last[k : k + 1, at + 256 : at + 384] for k in range(4)]
        extra = [
            hi, mid, last[:, at : at + 256],
            jnp.concatenate(ends_of[:2], axis=1), jnp.concatenate(ends_of[2:], axis=1),
        ]
        p_ref[slot, STATE:, :] = jnp.concatenate(extra, axis=0).astype(BF16)


CONV_AT = (0, 256, 640, 896)


def conv(rows, before, weight, bias, cols, mask):
    def whole(height, width, first):
        return pl.BlockSpec((1, height, width), lambda g, p: (0, 0, first + g))

    def flat(height, width, first):
        return pl.BlockSpec((height, width), lambda g, p: (0, first + g))

    return pl.pallas_call(
        conv_kernel,
        grid_spec=pltpu.PrefetchScalarGridSpec(
            num_scalar_prefetch=1,
            grid=(GROUPS,),
            in_specs=[
                whole(L_DEV, GROUP_CH, 0), whole(L_DEV, 128, 32),
                whole(3, GROUP_CH, 0), whole(3, 128, 32),
                flat(4, GROUP_CH, 0), flat(4, 128, 32),
                flat(1, GROUP_CH, 0), flat(1, 128, 32),
                pl.BlockSpec((1, 16, CH // GROUPS), lambda g, p: (0, L_DEV // 16 - 1, g)),
                pl.BlockSpec((1, L_DEV, 128), lambda g, p: (g, 0, 0)),
            ],
            out_specs=(
                flat(L_DEV, GROUP_CH, 0),
                flat(L_DEV, 128, 0),
                pl.BlockSpec((1, STATE, GROUP_CH), lambda g, p: (g, 0, 0)),
                pl.BlockSpec((4, SENT_ROWS, OWN_CH), lambda g, p: (g ^ (p[0] // 4), 0, 0)),
            ),
            scratch_shapes=[
                pltpu.VMEM((9, L_DEV + 8, 128), F32),
                pltpu.VMEM((L_DEV, GROUP_CH), BF16),
                pltpu.VMEM((4, L_DEV, OWN_CH), F32),
                pltpu.VMEM((128, GROUP_CH), BF16),
                pltpu.VMEM((128, GROUP_CH), BF16),
            ],
        ),
        out_shape=(
            jax.ShapeDtypeStruct((L_DEV, D_IN), BF16),
            jax.ShapeDtypeStruct((L_DEV, GROUPS * STATE), BF16),
            jax.ShapeDtypeStruct((GROUPS, STATE, GROUP_CH), BF16),
            jax.ShapeDtypeStruct((SHARDS, SENT_ROWS, OWN_CH), BF16),
        ),
        cost_estimate=pl.CostEstimate(flops=10 * 10**9, bytes_accessed=14 * 2**20, transcendentals=0),
        compiler_params=pltpu.CompilerParams(vmem_limit_bytes=VMEM_LIMIT),
        name="conv_state",
    )(mask, rows, rows, before, before, weight, weight, bias, bias, rows, cols)


def intra_kernel(
    x_ref, b_ref, c_ref, hc_ref, wc_ref, bc_ref, row_ref, col_ref, y_ref, co_ref, cf
):
    half = BLOCK // 2
    j = pl.program_id(1)
    sums = pltpu.roll(col_ref[...], (GROUPS - pl.program_id(0)) * PER_GROUP, 1)

    @pl.when(j == 0)
    def _():
        cf[5:8, :] = hc_ref[0].astype(F32)

    @pl.when(j == 1)
    def _():
        cf[0:8, :] = cf[BLOCK : BLOCK + 8, :]

    cf[8 : 8 + BLOCK, :] = c_ref[0].astype(F32)
    w, bias = taps(wc_ref, bc_ref, slice(0, 128))
    for r0 in range(0, BLOCK, CONV_ROWS):
        co_ref[r0 : r0 + CONV_ROWS, :] = silu_of(cf, 5 + r0, w, bias).astype(BF16)
    scores = lax.dot_general(
        co_ref[...], b_ref[...], (((1,), (1,)), ((), ())), preferred_element_type=F32
    )
    t = lax.broadcasted_iota(jnp.int32, (half, half), 0)
    u = lax.broadcasted_iota(jnp.int32, (half, half), 1)
    s00 = jnp.where(u <= t, scores[:half, :half], 0.0)
    s10 = scores[half:, :half]
    s11 = jnp.where(u <= t, scores[half:, half:], 0.0)
    low = lax.broadcasted_iota(jnp.int32, (BLOCK, 128), 1) < HEAD_DIM
    for pair in range(PER_GROUP // 2):
        lanes = slice(pair * 128, (pair + 1) * 128)
        x = x_ref[:, lanes]
        zero = jnp.zeros_like(x)
        xl, xh = jnp.where(low, x, zero), jnp.where(low, zero, x)
        top, bottom = [], []
        for h in (2 * pair, 2 * pair + 1):
            cs0 = jnp.broadcast_to(sums[:half, h : h + 1], (half, half))
            cs1 = jnp.broadcast_to(sums[half:, h : h + 1], (half, half))
            a0 = row_ref[h : h + 1, :half]
            a1 = row_ref[h : h + 1, half:]
            top.append((jnp.exp2(jnp.minimum(cs0 - a0, CAP)) * s00).astype(BF16))
            bottom.append((jnp.exp2(cs1 - a0) * s10).astype(BF16))
            bottom.append((jnp.exp2(jnp.minimum(cs1 - a1, CAP)) * s11).astype(BF16))
        above = dot(jnp.concatenate(top, axis=1), jnp.concatenate([xl[:half], xh[:half]], axis=0))
        below = dot(jnp.concatenate(bottom, axis=1), jnp.concatenate([xl, xh], axis=0))
        y_ref[:half, lanes] = above.astype(BF16)
        y_ref[half:, lanes] = below.astype(BF16)


def intra(x, b, rows, before, weight, bias, starts, sums):
    def at_c(g, j):
        return (0, D_IN // 128 + GROUPS + g)

    return pl.pallas_call(
        intra_kernel,
        grid=(GROUPS, L_DEV // BLOCK),
        in_specs=[
            pl.BlockSpec((BLOCK, GROUP_CH), lambda g, j: (j, g)),
            pl.BlockSpec((BLOCK, 128), lambda g, j: (j, g)),
            pl.BlockSpec((1, BLOCK, 128), lambda g, j: (0, j, at_c(g, j)[1])),
            pl.BlockSpec((1, 3, 128), lambda g, j: (0, 0, at_c(g, j)[1])),
            pl.BlockSpec((4, 128), at_c),
            pl.BlockSpec((1, 128), at_c),
            pl.BlockSpec((PER_GROUP, BLOCK), lambda g, j: (g, j)),
            pl.BlockSpec((BLOCK, 2 * HEADS), lambda g, j: (j, 0)),
        ],
        out_specs=(
            pl.BlockSpec((BLOCK, GROUP_CH), lambda g, j: (j, g)),
            pl.BlockSpec((BLOCK, 128), lambda g, j: (j, g)),
        ),
        out_shape=(
            jax.ShapeDtypeStruct((L_DEV, D_IN), BF16),
            jax.ShapeDtypeStruct((L_DEV, GROUPS * STATE), BF16),
        ),
        scratch_shapes=[pltpu.VMEM((BLOCK + 8, 128), F32)],
        cost_estimate=pl.CostEstimate(flops=12 * 10**9, bytes_accessed=12 * 2**20, transcendentals=0),
        compiler_params=pltpu.CompilerParams(vmem_limit_bytes=VMEM_LIMIT),
        name="intra",
    )(x, b, rows, before, weight, bias, starts, sums)


def scan_kernel(r_ref, p_ref, piece_ref):
    state = jnp.zeros((STATE, OWN_CH), F32)
    for d in range(SHARDS):
        slot = d ^ FLIP
        p_ref[slot] = state.astype(BF16)
        extra = r_ref[slot, STATE:, :].astype(F32)
        state = (extra[0:1] + extra[1:2]) * state + r_ref[slot, :STATE, :].astype(F32)
    size = STATE // PIECES
    zero = jnp.zeros((PIECE_ROWS - size - 3, OWN_CH), F32)
    for k in range(PIECES):
        rows = extra[2 + 2 * k : 4 + 2 * k]
        parts = [state[k * size : k * size + size], rows, extra[6 + k : 7 + k], zero]
        piece_ref[k * PIECE_ROWS : (k + 1) * PIECE_ROWS, :] = jnp.concatenate(parts, axis=0).astype(BF16)


def scan(got):
    return pl.pallas_call(
        scan_kernel,
        out_shape=(
            jax.ShapeDtypeStruct((SHARDS, STATE, OWN_CH), BF16),
            jax.ShapeDtypeStruct((PIECES * PIECE_ROWS, OWN_CH), BF16),
        ),
        cost_estimate=pl.CostEstimate(flops=10**9, bytes_accessed=2**22, transcendentals=0),
        compiler_params=pltpu.CompilerParams(vmem_limit_bytes=VMEM_LIMIT),
        name="scan",
    )(got)


def pack_kernel(place_ref, prompt_ref, owner_ref, *refs):
    pieces, p_ref = refs[:-1], refs[-1]
    p_ref[...] = jnp.zeros_like(p_ref)
    for k in range(PIECES):
        p_ref[owner_ref[place_ref[0] ^ prompt_ref[0] ^ k] ^ FLIP] = pieces[k][...]


def pack(place, prompt, owner_slot, pieces):
    return pl.pallas_call(
        pack_kernel,
        in_specs=[SMEM] * 3 + [VMEM] * PIECES,
        out_shape=jax.ShapeDtypeStruct((SHARDS, PIECE_ROWS, OWN_CH), BF16),
        cost_estimate=pl.CostEstimate(flops=10**8, bytes_accessed=2**19, transcendentals=0),
        compiler_params=pltpu.CompilerParams(vmem_limit_bytes=VMEM_LIMIT),
        name="pack",
    )(place, prompt, owner_slot, *pieces)


def unpack_kernel(place_ref, prompt_ref, owner_ref, r_ref, ssm_ref, conv_ref):
    size = STATE // PIECES
    mine = 0
    for p in range(SHARDS):
        mine = jnp.where(owner_ref[p] == place_ref[0], p, mine)
    parts = [r_ref[mine ^ prompt_ref[0] ^ k ^ FLIP].astype(F32) for k in range(PIECES)]
    state = jnp.concatenate([part[:size] for part in parts], axis=0)
    ssm_ref[...] = jnp.transpose(state)
    rows = jnp.concatenate([part[size : size + 2] for part in parts], axis=0)
    ends = [part[size + 2 : size + 3, n * 128 : n * 128 + 128] for part in parts for n in range(2)]
    window = jnp.concatenate([rows, jnp.concatenate(ends, axis=0)], axis=1)
    moved = jnp.concatenate([window[:, 64:], window[:, :64]], axis=1)
    odd = prompt_ref[0] % 2 == 1
    conv_ref[...] = jnp.where(odd, moved, window)[:, : CH // SHARDS].astype(BF16)


def unpack(place, prompt, owner_slot, got):
    return pl.pallas_call(
        unpack_kernel,
        in_specs=[SMEM] * 3 + [VMEM],
        out_shape=(
            jax.ShapeDtypeStruct((OWN_CH, STATE), F32),
            jax.ShapeDtypeStruct((4, CH // SHARDS), BF16),
        ),
        cost_estimate=pl.CostEstimate(flops=10**8, bytes_accessed=2**19, transcendentals=0),
        compiler_params=pltpu.CompilerParams(vmem_limit_bytes=VMEM_LIMIT),
        name="unpack",
    )(place, prompt, owner_slot, got)


def out_kernel(mask_ref, y_ref, c_ref, col_ref, e0_ref, state_ref, gain_ref, o_ref, ys, spread):
    within = mask_ref[0] % 4

    @pl.when(pl.program_id(0) == 0)
    def _():
        spread[...] = spread_matrix(GROWN)

    decay = dot(col_ref[0, 240:256, :], spread[...])[15:16]
    for j in range(2):
        rows = slice(j * BLOCK, (j + 1) * BLOCK)
        c = c_ref[rows, :]
        grown = col_ref[0, rows, :]
        total = jnp.zeros((BLOCK, 128), F32)
        for s in range(4):
            lanes = slice(s * OWN_CH, (s + 1) * OWN_CH)
            state = state_ref[s ^ within]
            if j == 1:
                state = (decay[:, lanes] * state.astype(F32) + e0_ref[0, :, lanes].astype(F32)).astype(BF16)
            y = y_ref[rows, lanes].astype(F32) + dot(grown, spread[:, lanes]) * dot(c, state)
            ys[:, lanes] = y
            total = total + y[:, :128] * y[:, :128] + y[:, 128:] * y[:, 128:]
        mean = jnp.sum(total, axis=1, keepdims=True) * (1.0 / GROUP_CH)
        scale = lax.rsqrt(mean + NORM_EPS)
        o_ref[0, rows, :] = (ys[...] * scale * gain_ref[...]).astype(BF16)


def finish(y, c, cols, e0, states, gain, mask):
    return pl.pallas_call(
        out_kernel,
        grid_spec=pltpu.PrefetchScalarGridSpec(
            num_scalar_prefetch=1,
            grid=(GROUPS,),
            in_specs=[
                pl.BlockSpec((L_DEV, GROUP_CH), lambda g, m: (0, g)),
                pl.BlockSpec((L_DEV, 128), lambda g, m: (0, g)),
                pl.BlockSpec((1, L_DEV, 128), lambda g, m: (g, 0, 0)),
                pl.BlockSpec((1, STATE, GROUP_CH), lambda g, m: (g, 0, 0)),
                pl.BlockSpec((4, STATE, OWN_CH), lambda g, m: (g ^ (m[0] // 4), 0, 0)),
                pl.BlockSpec((1, GROUP_CH), lambda g, m: (0, g)),
            ],
            out_specs=pl.BlockSpec((1, L_DEV, GROUP_CH), lambda g, m: (0, 0, g)),
            scratch_shapes=[pltpu.VMEM((BLOCK, GROUP_CH), F32), pltpu.VMEM((128, GROUP_CH), BF16)],
        ),
        out_shape=jax.ShapeDtypeStruct((1, L_DEV, D_IN), BF16),
        cost_estimate=pl.CostEstimate(flops=8 * 10**9, bytes_accessed=12 * 2**20, transcendentals=0),
        compiler_params=pltpu.CompilerParams(vmem_limit_bytes=VMEM_LIMIT),
        name="finish",
    )(mask, y, c, cols, e0, states, gain)


def exchange(pieces):
    groups = [[(r ^ FLIP) * SHARDS + p for r in range(SHARDS)] for p in range(SHARDS)]
    return lax.all_to_all(
        pieces, ("seq", "grp"), split_axis=0, concat_axis=0, tiled=True, axis_index_groups=groups
    )


def body(conv_input, step_raw, decay_rate, conv_weight, conv_bias, norm_gain, owner_slot):
    place = lax.axis_index("seq").astype(jnp.int32)[None]
    prompt = lax.axis_index("grp").astype(jnp.int32)[None]
    route = [(d, d + 1) for d in range(SHARDS - 1)]
    before = lax.ppermute(conv_input[:, L_DEV - 3 :, :], "seq", route)
    starts, sums, cols = prep(step_raw, decay_rate[None, :])
    bias = conv_bias[None, :]
    x, b, e0, sent = conv(conv_input, before, conv_weight, bias, cols, prompt ^ FLIP)
    y, c = intra(x, b, conv_input, before, conv_weight, bias, starts, sums)
    got, y = lax.optimization_barrier((exchange(sent), y))
    states, final = scan(got)
    entering = exchange(states)
    turn = [
        (r * SHARDS + p, r * SHARDS + (r ^ p)) for r in range(SHARDS) for p in range(SHARDS)
    ]
    final = lax.ppermute(final, ("seq", "grp"), turn)
    kept, passed = final[:PIECE_ROWS], final[PIECE_ROWS:]
    pieces = [kept, lax.ppermute(passed, "seq", [(r, r ^ 1) for r in range(SHARDS)])]
    packed = pack(place, prompt, owner_slot, pieces)
    entering, packed = lax.optimization_barrier((entering, packed))
    arrived = exchange(packed)
    mixed = finish(y, c, cols, e0, entering, norm_gain[None, :], prompt ^ FLIP)
    ssm, rows = unpack(place, prompt, owner_slot, arrived)
    return mixed, ssm.reshape(1, 4, HEAD_DIM, STATE), jnp.transpose(rows)[None]


def solution(mesh):
    return jax.shard_map(
        body,
        mesh=mesh,
        in_specs=(P("grp", "seq", None), P("grp", None, "seq"), P(), P(), P(), P(), P()),
        out_specs=(P("grp", "seq", None), P("seq", "grp", None, None), P("seq", "grp", None)),
        check_vma=False,
    )
```

```python
import functools
import math

import jax
import jax.numpy as jnp
from jax import lax
from jax.experimental import pallas as pl
from jax.experimental.pallas import tpu as pltpu
from jax.sharding import PartitionSpec as P

HEADS = 64
HEAD_DIM = 64
STATE = 128
GROUPS = 4
PER_GROUP = HEADS // GROUPS
GROUP_CH = PER_GROUP * HEAD_DIM
BLOCK = 256
D_IN = 4096
CH = 5120
L_DEV = 512
SHARDS = 16
OWN_CH = 256
SENT_ROWS = 136
PIECES = 2
FLIP = SHARDS - 1
PIECE_ROWS = 72
VMEM_LIMIT = 67043328
NORM_EPS = 1.0
LOG2E = math.log2(math.e)
CAP = 64.0

SMEM = pl.BlockSpec(memory_space=pltpu.SMEM)
VMEM = pl.BlockSpec(memory_space=pltpu.VMEM)
ANY = pl.BlockSpec(memory_space=pl.ANY)

F32 = jnp.float32
BF16 = jnp.bfloat16


def dot(a, b):
    return lax.dot_general(a, b, (((1,), (0,)), ((), ())), preferred_element_type=F32)


def three_pieces(v):
    hi = v.astype(BF16).astype(F32)
    rest = v - hi
    mid = rest.astype(BF16).astype(F32)
    return hi, mid, (rest - mid).astype(BF16).astype(F32)


TAIL, GROWN = 0, 48


def spread_matrix(first):
    row = lax.broadcasted_iota(jnp.int32, (128, GROUP_CH), 0)
    col = lax.broadcasted_iota(jnp.int32, (128, GROUP_CH), 1)
    hit = (row >= first) & (row < first + 48) & (row % PER_GROUP == col // HEAD_DIM)
    return jnp.where(hit, 1.0, 0.0).astype(BF16)


def prep_kernel(step_ref, rate_ref, row_ref, sum_ref, col_ref):
    dt = jax.nn.softplus(step_ref[0])
    near = lax.broadcasted_iota(jnp.int32, (HEADS, HEADS), 0)
    far = lax.broadcasted_iota(jnp.int32, (HEADS, HEADS), 1)
    decay = jnp.sum(jnp.where(near == far, rate_ref[...], 0.0), axis=1, keepdims=True)
    rate = dt * (decay * -LOG2E)
    later = lax.broadcasted_iota(jnp.int32, (BLOCK, BLOCK), 0)
    earlier = lax.broadcasted_iota(jnp.int32, (BLOCK, BLOCK), 1)
    upto = jnp.where(later <= earlier, 1.0, 0.0).astype(BF16)
    zero = jnp.zeros((2 * PER_GROUP, BLOCK), F32)
    for j in range(L_DEV // BLOCK):
        span = slice(j * BLOCK, (j + 1) * BLOCK)
        dt_j = dt[:, span]
        stacked = jnp.concatenate(three_pieces(rate[:, span]), axis=0).astype(BF16)
        sums = dot(stacked, upto)
        cs = sums[:HEADS] + sums[HEADS : 2 * HEADS] + sums[2 * HEADS :]
        row_ref[:, span] = cs - jnp.log2(dt_j)
        tail = three_pieces(jnp.exp2(cs[:, BLOCK - 1 :] - cs) * dt_j)
        grown = three_pieces(jnp.exp2(cs))
        sum_ref[span, :] = jnp.transpose(jnp.concatenate([cs, cs], axis=0))
        for g in range(GROUPS):
            heads = slice(g * PER_GROUP, (g + 1) * PER_GROUP)
            parts = [v[heads] for v in tail + grown] + [zero]
            col_ref[g, span, :] = jnp.transpose(jnp.concatenate(parts, axis=0)).astype(BF16)


def prep(step_raw, decay_rate):
    return pl.pallas_call(
        prep_kernel,
        out_shape=(
            jax.ShapeDtypeStruct((HEADS, L_DEV), F32),
            jax.ShapeDtypeStruct((L_DEV, 2 * HEADS), F32),
            jax.ShapeDtypeStruct((GROUPS, L_DEV, 128), BF16),
        ),
        cost_estimate=pl.CostEstimate(flops=10**9, bytes_accessed=2**21, transcendentals=0),
        compiler_params=pltpu.CompilerParams(vmem_limit_bytes=VMEM_LIMIT),
        name="prep",
    )(step_raw, decay_rate)


CONV_ROWS = 16


def taps(w_ref, bias_ref, lanes):
    w = w_ref[:, lanes].astype(F32) * 0.5
    return [w[k : k + 1] for k in range(4)], bias_ref[:, lanes].astype(F32) * 0.5


def silu_of(values, at, w, bias):
    half = bias + w[0] * values[at : at + CONV_ROWS, :]
    for k in range(1, 4):
        half = half + w[k] * values[at + k : at + k + CONV_ROWS, :]
    return half + half * jnp.tanh(half)


def conv_kernel(
    mask_ref, x_ref, b_ref, hx_ref, hb_ref, wx_ref, wb_ref, bx_ref, bb_ref, last_ref, col_ref,
    xo_ref, bo_ref, e0_ref, p_ref, xf, xs, tails, spread, regrown,
):
    within = mask_ref[0] % 4

    @pl.when(pl.program_id(0) == 0)
    def _():
        spread[...] = spread_matrix(TAIL)
        regrown[...] = spread_matrix(GROWN)

    def load(slot, ref, halo_ref, lanes):
        xf[slot, 5:8, :] = halo_ref[0, :, lanes].astype(F32)
        xf[slot, 8 : 8 + L_DEV, :] = ref[0, :, lanes].astype(F32)

    load(8, b_ref, hb_ref, slice(0, 128))
    w, bias = taps(wb_ref, bb_ref, slice(0, 128))
    for r0 in range(0, L_DEV, CONV_ROWS):
        bo_ref[r0 : r0 + CONV_ROWS, :] = silu_of(xf.at[8], 5 + r0, w, bias).astype(BF16)
    bt = [
        jnp.transpose(bo_ref[j * BLOCK : (j + 1) * BLOCK, :].astype(F32)).astype(BF16) for j in range(2)
    ]
    ends = jnp.concatenate([col_ref[0, 240:256, :], col_ref[0, 496:512, :]], axis=0)
    decays = dot(ends, regrown[...])
    last = last_ref[0].astype(F32)[12:16]
    def widen(s):
        tails[s] = dot(col_ref[0], spread[:, s * OWN_CH : (s + 1) * OWN_CH])

    def emit(s):
        wide = slice(s * OWN_CH, (s + 1) * OWN_CH)
        first, second = decays[15:16, wide], decays[31:32, wide]
        e0 = dot(bt[0], xs[:BLOCK, wide])
        e1 = dot(bt[1], xs[BLOCK:, wide])
        e0_ref[0, :, wide] = e0.astype(BF16)
        slot = s ^ within
        p_ref[slot, :STATE, :] = (second * e0 + e1).astype(BF16)
        hi, mid, _ = three_pieces(first * second)
        at = CONV_AT[s]
        ends_of = [last[k : k + 1, at + 256 : at + 384] for k in range(4)]
        extra = [
            hi, mid, last[:, at : at + 256],
            jnp.concatenate(ends_of[:2], axis=1), jnp.concatenate(ends_of[2:], axis=1),
        ]
        p_ref[slot, STATE:, :] = jnp.concatenate(extra, axis=0).astype(BF16)

    widen(0)
    for s in range(4):
        wide = slice(s * OWN_CH, (s + 1) * OWN_CH)
        pair = (2 * s, 2 * s + 1)
        both = []
        for k in pair:
            lanes = slice(k * 128, (k + 1) * 128)
            load(k, x_ref, hx_ref, lanes)
            both.append(taps(wx_ref, bx_ref, lanes))
        for r0 in range(0, L_DEV, CONV_ROWS):
            if r0 == 0 and s < 3:
                widen(s + 1)
            if r0 == 0 and s > 0:
                emit(s - 1)
            rows = slice(r0, r0 + CONV_ROWS)
            parts = [silu_of(xf.at[k], 5 + r0, *tap) for k, tap in zip(pair, both)]
            value = jnp.concatenate(parts, axis=1)
            xo_ref[rows, wide] = value.astype(BF16)
            xs[rows, wide] = (value * tails[s, rows, :]).astype(BF16)
    emit(3)


CONV_AT = (0, 256, 640, 896)


def conv(rows, before, weight, bias, cols, mask):
    def whole(height, width, first):
        return pl.BlockSpec((1, height, width), lambda g, p: (0, 0, first + g))

    def flat(height, width, first):
        return pl.BlockSpec((height, width), lambda g, p: (0, first + g))

    return pl.pallas_call(
        conv_kernel,
        grid_spec=pltpu.PrefetchScalarGridSpec(
            num_scalar_prefetch=1,
            grid=(GROUPS,),
            in_specs=[
                whole(L_DEV, GROUP_CH, 0), whole(L_DEV, 128, 32),
                whole(3, GROUP_CH, 0), whole(3, 128, 32),
                flat(4, GROUP_CH, 0), flat(4, 128, 32),
                flat(1, GROUP_CH, 0), flat(1, 128, 32),
                pl.BlockSpec((1, 16, CH // GROUPS), lambda g, p: (0, L_DEV // 16 - 1, g)),
                pl.BlockSpec((1, L_DEV, 128), lambda g, p: (g, 0, 0)),
            ],
            out_specs=(
                flat(L_DEV, GROUP_CH, 0),
                flat(L_DEV, 128, 0),
                pl.BlockSpec((1, STATE, GROUP_CH), lambda g, p: (g, 0, 0)),
                pl.BlockSpec((4, SENT_ROWS, OWN_CH), lambda g, p: (g ^ (p[0] // 4), 0, 0)),
            ),
            scratch_shapes=[
                pltpu.VMEM((9, L_DEV + 8, 128), F32),
                pltpu.VMEM((L_DEV, GROUP_CH), BF16),
                pltpu.VMEM((4, L_DEV, OWN_CH), F32),
                pltpu.VMEM((128, GROUP_CH), BF16),
                pltpu.VMEM((128, GROUP_CH), BF16),
            ],
        ),
        out_shape=(
            jax.ShapeDtypeStruct((L_DEV, D_IN), BF16),
            jax.ShapeDtypeStruct((L_DEV, GROUPS * STATE), BF16),
            jax.ShapeDtypeStruct((GROUPS, STATE, GROUP_CH), BF16),
            jax.ShapeDtypeStruct((SHARDS, SENT_ROWS, OWN_CH), BF16),
        ),
        cost_estimate=pl.CostEstimate(flops=10 * 10**9, bytes_accessed=14 * 2**20, transcendentals=0),
        compiler_params=pltpu.CompilerParams(vmem_limit_bytes=VMEM_LIMIT),
        name="conv_state",
    )(mask, rows, rows, before, before, weight, weight, bias, bias, rows, cols)


def intra_kernel(
    x_ref, b_ref, c_ref, hc_ref, wc_ref, bc_ref, row_ref, col_ref, y_ref, co_ref, cf
):
    half = BLOCK // 2
    j = pl.program_id(1)
    sums = pltpu.roll(col_ref[...], (GROUPS - pl.program_id(0)) * PER_GROUP, 1)

    @pl.when(j == 0)
    def _():
        cf[5:8, :] = hc_ref[0].astype(F32)

    @pl.when(j == 1)
    def _():
        cf[0:8, :] = cf[BLOCK : BLOCK + 8, :]

    cf[8 : 8 + BLOCK, :] = c_ref[0].astype(F32)
    w, bias = taps(wc_ref, bc_ref, slice(0, 128))
    for r0 in range(0, BLOCK, CONV_ROWS):
        co_ref[r0 : r0 + CONV_ROWS, :] = silu_of(cf, 5 + r0, w, bias).astype(BF16)
    scores = lax.dot_general(
        co_ref[...], b_ref[...], (((1,), (1,)), ((), ())), preferred_element_type=F32
    )
    t = lax.broadcasted_iota(jnp.int32, (half, half), 0)
    u = lax.broadcasted_iota(jnp.int32, (half, half), 1)
    s00 = jnp.where(u <= t, scores[:half, :half], 0.0)
    s10 = scores[half:, :half]
    s11 = jnp.where(u <= t, scores[half:, half:], 0.0)
    low = lax.broadcasted_iota(jnp.int32, (BLOCK, 128), 1) < HEAD_DIM
    for pair in range(PER_GROUP // 2):
        lanes = slice(pair * 128, (pair + 1) * 128)
        x = x_ref[:, lanes]
        zero = jnp.zeros_like(x)
        xl, xh = jnp.where(low, x, zero), jnp.where(low, zero, x)
        top, bottom = [], []
        for h in (2 * pair, 2 * pair + 1):
            cs0 = jnp.broadcast_to(sums[:half, h : h + 1], (half, half))
            cs1 = jnp.broadcast_to(sums[half:, h : h + 1], (half, half))
            a0 = row_ref[h : h + 1, :half]
            a1 = row_ref[h : h + 1, half:]
            top.append((jnp.exp2(jnp.minimum(cs0 - a0, CAP)) * s00).astype(BF16))
            bottom.append((jnp.exp2(cs1 - a0) * s10).astype(BF16))
            bottom.append((jnp.exp2(jnp.minimum(cs1 - a1, CAP)) * s11).astype(BF16))
        above = dot(jnp.concatenate(top, axis=1), jnp.concatenate([xl[:half], xh[:half]], axis=0))
        below = dot(jnp.concatenate(bottom, axis=1), jnp.concatenate([xl, xh], axis=0))
        y_ref[:half, lanes] = above.astype(BF16)
        y_ref[half:, lanes] = below.astype(BF16)


def intra(x, b, rows, before, weight, bias, starts, sums):
    def at_c(g, j):
        return (0, D_IN // 128 + GROUPS + g)

    return pl.pallas_call(
        intra_kernel,
        grid=(GROUPS, L_DEV // BLOCK),
        in_specs=[
            pl.BlockSpec((BLOCK, GROUP_CH), lambda g, j: (j, g)),
            pl.BlockSpec((BLOCK, 128), lambda g, j: (j, g)),
            pl.BlockSpec((1, BLOCK, 128), lambda g, j: (0, j, at_c(g, j)[1])),
            pl.BlockSpec((1, 3, 128), lambda g, j: (0, 0, at_c(g, j)[1])),
            pl.BlockSpec((4, 128), at_c),
            pl.BlockSpec((1, 128), at_c),
            pl.BlockSpec((PER_GROUP, BLOCK), lambda g, j: (g, j)),
            pl.BlockSpec((BLOCK, 2 * HEADS), lambda g, j: (j, 0)),
        ],
        out_specs=(
            pl.BlockSpec((BLOCK, GROUP_CH), lambda g, j: (j, g)),
            pl.BlockSpec((BLOCK, 128), lambda g, j: (j, g)),
        ),
        out_shape=(
            jax.ShapeDtypeStruct((L_DEV, D_IN), BF16),
            jax.ShapeDtypeStruct((L_DEV, GROUPS * STATE), BF16),
        ),
        scratch_shapes=[pltpu.VMEM((BLOCK + 8, 128), F32)],
        cost_estimate=pl.CostEstimate(flops=12 * 10**9, bytes_accessed=12 * 2**20, transcendentals=0),
        compiler_params=pltpu.CompilerParams(vmem_limit_bytes=VMEM_LIMIT),
        name="intra",
    )(x, b, rows, before, weight, bias, starts, sums)


def scan_kernel(r_ref, p_ref, piece_ref):
    state = jnp.zeros((STATE, r_ref.shape[-1]), F32)
    for d in range(SHARDS):
        slot = d ^ FLIP
        p_ref[slot] = state.astype(BF16)
        extra = r_ref[slot, STATE:, :].astype(F32)
        state = (extra[0:1] + extra[1:2]) * state + r_ref[slot, :STATE, :].astype(F32)
    size = STATE // PIECES
    zero = jnp.zeros((PIECE_ROWS - size - 3, r_ref.shape[-1]), F32)
    for k in range(PIECES):
        rows = extra[2 + 2 * k : 4 + 2 * k]
        parts = [state[k * size : k * size + size], rows, extra[6 + k : 7 + k], zero]
        piece_ref[k * PIECE_ROWS : (k + 1) * PIECE_ROWS, :] = jnp.concatenate(parts, axis=0).astype(BF16)


def scan(got):
    return pl.pallas_call(
        scan_kernel,
        grid=(OWN_CH // 128,),
        in_specs=[pl.BlockSpec((SHARDS, SENT_ROWS, 128), lambda i: (0, 0, i))],
        out_specs=(
            pl.BlockSpec((SHARDS, STATE, 128), lambda i: (0, 0, i)),
            pl.BlockSpec((PIECES * PIECE_ROWS, 128), lambda i: (0, i)),
        ),
        out_shape=(
            jax.ShapeDtypeStruct((SHARDS, STATE, OWN_CH), BF16),
            jax.ShapeDtypeStruct((PIECES * PIECE_ROWS, OWN_CH), BF16),
        ),
        cost_estimate=pl.CostEstimate(flops=10**9, bytes_accessed=2**22, transcendentals=0),
        compiler_params=pltpu.CompilerParams(vmem_limit_bytes=VMEM_LIMIT),
        name="scan",
    )(got)


def pack_kernel(place_ref, prompt_ref, owner_ref, *refs):
    pieces, p_ref = refs[:-1], refs[-1]
    p_ref[...] = jnp.zeros_like(p_ref)
    for k in range(PIECES):
        p_ref[owner_ref[place_ref[0] ^ prompt_ref[0] ^ k] ^ FLIP] = pieces[k][...]


def pack(place, prompt, owner_slot, pieces):
    return pl.pallas_call(
        pack_kernel,
        in_specs=[SMEM] * 3 + [VMEM] * PIECES,
        out_shape=jax.ShapeDtypeStruct((SHARDS, PIECE_ROWS, OWN_CH), BF16),
        cost_estimate=pl.CostEstimate(flops=10**8, bytes_accessed=2**19, transcendentals=0),
        compiler_params=pltpu.CompilerParams(vmem_limit_bytes=VMEM_LIMIT),
        name="pack",
    )(place, prompt, owner_slot, *pieces)


def unpack_kernel(place_ref, prompt_ref, owner_ref, r_ref, ssm_ref, conv_ref):
    size = STATE // PIECES
    mine = 0
    for p in range(SHARDS):
        mine = jnp.where(owner_ref[p] == place_ref[0], p, mine)
    parts = [r_ref[mine ^ prompt_ref[0] ^ k ^ FLIP].astype(F32) for k in range(PIECES)]
    state = jnp.concatenate([part[:size] for part in parts], axis=0)
    ssm_ref[...] = jnp.transpose(state)
    rows = jnp.concatenate([part[size : size + 2] for part in parts], axis=0)
    ends = [part[size + 2 : size + 3, n * 128 : n * 128 + 128] for part in parts for n in range(2)]
    window = jnp.concatenate([rows, jnp.concatenate(ends, axis=0)], axis=1)
    moved = jnp.concatenate([window[:, 64:], window[:, :64]], axis=1)
    odd = prompt_ref[0] % 2 == 1
    conv_ref[...] = jnp.where(odd, moved, window)[:, : CH // SHARDS].astype(BF16)


def unpack(place, prompt, owner_slot, got):
    return pl.pallas_call(
        unpack_kernel,
        in_specs=[SMEM] * 3 + [VMEM],
        out_shape=(
            jax.ShapeDtypeStruct((OWN_CH, STATE), F32),
            jax.ShapeDtypeStruct((4, CH // SHARDS), BF16),
        ),
        cost_estimate=pl.CostEstimate(flops=10**8, bytes_accessed=2**19, transcendentals=0),
        compiler_params=pltpu.CompilerParams(vmem_limit_bytes=VMEM_LIMIT),
        name="unpack",
    )(place, prompt, owner_slot, got)


def out_kernel(mask_ref, y_ref, c_ref, col_ref, e0_ref, state_ref, gain_ref, o_ref, ys, spread):
    within = mask_ref[0] % 4

    @pl.when(pl.program_id(0) == 0)
    def _():
        spread[...] = spread_matrix(GROWN)

    decay = dot(col_ref[0, 240:256, :], spread[...])[15:16]
    for j in range(2):
        rows = slice(j * BLOCK, (j + 1) * BLOCK)
        c = c_ref[rows, :]
        grown = col_ref[0, rows, :]
        total = jnp.zeros((BLOCK, 128), F32)
        for s in range(4):
            lanes = slice(s * OWN_CH, (s + 1) * OWN_CH)
            state = state_ref[s ^ within]
            if j == 1:
                state = (decay[:, lanes] * state.astype(F32) + e0_ref[0, :, lanes].astype(F32)).astype(BF16)
            y = y_ref[rows, lanes].astype(F32) + dot(grown, spread[:, lanes]) * dot(c, state)
            ys[:, lanes] = y
            total = total + y[:, :128] * y[:, :128] + y[:, 128:] * y[:, 128:]
        mean = jnp.sum(total, axis=1, keepdims=True) * (1.0 / GROUP_CH)
        scale = lax.rsqrt(mean + NORM_EPS)
        o_ref[0, rows, :] = (ys[...] * scale * gain_ref[...]).astype(BF16)


def finish(y, c, cols, e0, states, gain, mask):
    return pl.pallas_call(
        out_kernel,
        grid_spec=pltpu.PrefetchScalarGridSpec(
            num_scalar_prefetch=1,
            grid=(GROUPS,),
            in_specs=[
                pl.BlockSpec((L_DEV, GROUP_CH), lambda g, m: (0, g)),
                pl.BlockSpec((L_DEV, 128), lambda g, m: (0, g)),
                pl.BlockSpec((1, L_DEV, 128), lambda g, m: (g, 0, 0)),
                pl.BlockSpec((1, STATE, GROUP_CH), lambda g, m: (g, 0, 0)),
                pl.BlockSpec((4, STATE, OWN_CH), lambda g, m: (g ^ (m[0] // 4), 0, 0)),
                pl.BlockSpec((1, GROUP_CH), lambda g, m: (0, g)),
            ],
            out_specs=pl.BlockSpec((1, L_DEV, GROUP_CH), lambda g, m: (0, 0, g)),
            scratch_shapes=[pltpu.VMEM((BLOCK, GROUP_CH), F32), pltpu.VMEM((128, GROUP_CH), BF16)],
        ),
        out_shape=jax.ShapeDtypeStruct((1, L_DEV, D_IN), BF16),
        cost_estimate=pl.CostEstimate(flops=8 * 10**9, bytes_accessed=12 * 2**20, transcendentals=0),
        compiler_params=pltpu.CompilerParams(vmem_limit_bytes=VMEM_LIMIT),
        name="finish",
    )(mask, y, c, cols, e0, states, gain)


def exchange(pieces):
    groups = [[(r ^ FLIP) * SHARDS + p for r in range(SHARDS)] for p in range(SHARDS)]
    return lax.all_to_all(
        pieces, ("seq", "grp"), split_axis=0, concat_axis=0, tiled=True, axis_index_groups=groups
    )


def body(conv_input, step_raw, decay_rate, conv_weight, conv_bias, norm_gain, owner_slot):
    place = lax.axis_index("seq").astype(jnp.int32)[None]
    prompt = lax.axis_index("grp").astype(jnp.int32)[None]
    route = [(d, d + 1) for d in range(SHARDS - 1)]
    before = lax.ppermute(conv_input[:, L_DEV - 3 :, :], "seq", route)
    starts, sums, cols = prep(step_raw, decay_rate[None, :])
    bias = conv_bias[None, :]
    x, b, e0, sent = conv(conv_input, before, conv_weight, bias, cols, prompt ^ FLIP)
    y, c = intra(x, b, conv_input, before, conv_weight, bias, starts, sums)
    got, y = lax.optimization_barrier((exchange(sent), y))
    states, final = scan(got)
    entering = exchange(states)
    turn = [
        (r * SHARDS + p, r * SHARDS + (r ^ p)) for r in range(SHARDS) for p in range(SHARDS)
    ]
    final = lax.ppermute(final, ("seq", "grp"), turn)
    kept, passed = final[:PIECE_ROWS], final[PIECE_ROWS:]
    pieces = [kept, lax.ppermute(passed, "seq", [(r, r ^ 1) for r in range(SHARDS)])]
    packed = pack(place, prompt, owner_slot, pieces)
    entering, packed = lax.optimization_barrier((entering, packed))
    arrived = exchange(packed)
    mixed = finish(y, c, cols, e0, entering, norm_gain[None, :], prompt ^ FLIP)
    ssm, rows = unpack(place, prompt, owner_slot, arrived)
    return mixed, ssm.reshape(1, 4, HEAD_DIM, STATE), jnp.transpose(rows)[None]


def solution(mesh):
    return jax.shard_map(
        body,
        mesh=mesh,
        in_specs=(P("grp", "seq", None), P("grp", None, "seq"), P(), P(), P(), P(), P()),
        out_specs=(P("grp", "seq", None), P("seq", "grp", None, None), P("seq", "grp", None)),
        check_vma=False,
    )
```

```python
import functools
import math

import jax
import jax.numpy as jnp
from jax import lax
from jax.experimental import pallas as pl
from jax.experimental.pallas import tpu as pltpu
from jax.sharding import PartitionSpec as P

HEADS = 64
HEAD_DIM = 64
STATE = 128
GROUPS = 4
PER_GROUP = HEADS // GROUPS
GROUP_CH = PER_GROUP * HEAD_DIM
BLOCK = 256
D_IN = 4096
CH = 5120
L_DEV = 512
SHARDS = 16
OWN_CH = 256
SENT_ROWS = 136
PIECES = 2
FLIP = SHARDS - 1
PIECE_ROWS = 72
VMEM_LIMIT = 67043328
NORM_EPS = 1.0
LOG2E = math.log2(math.e)
CAP = 64.0

SMEM = pl.BlockSpec(memory_space=pltpu.SMEM)
VMEM = pl.BlockSpec(memory_space=pltpu.VMEM)
ANY = pl.BlockSpec(memory_space=pl.ANY)

F32 = jnp.float32
BF16 = jnp.bfloat16


def dot(a, b):
    return lax.dot_general(a, b, (((1,), (0,)), ((), ())), preferred_element_type=F32)


def three_pieces(v):
    hi = v.astype(BF16).astype(F32)
    rest = v - hi
    mid = rest.astype(BF16).astype(F32)
    return hi, mid, (rest - mid).astype(BF16).astype(F32)


TAIL, GROWN = 0, 48


def spread_matrix(first):
    row = lax.broadcasted_iota(jnp.int32, (128, GROUP_CH), 0)
    col = lax.broadcasted_iota(jnp.int32, (128, GROUP_CH), 1)
    hit = (row >= first) & (row < first + 48) & (row % PER_GROUP == col // HEAD_DIM)
    return jnp.where(hit, 1.0, 0.0).astype(BF16)


def prep_kernel(step_ref, rate_ref, row_ref, sum_ref, col_ref):
    dt = jax.nn.softplus(step_ref[0])
    near = lax.broadcasted_iota(jnp.int32, (HEADS, HEADS), 0)
    far = lax.broadcasted_iota(jnp.int32, (HEADS, HEADS), 1)
    decay = jnp.sum(jnp.where(near == far, rate_ref[...], 0.0), axis=1, keepdims=True)
    rate = dt * (decay * -LOG2E)
    later = lax.broadcasted_iota(jnp.int32, (BLOCK, BLOCK), 0)
    earlier = lax.broadcasted_iota(jnp.int32, (BLOCK, BLOCK), 1)
    upto = jnp.where(later <= earlier, 1.0, 0.0).astype(BF16)
    zero = jnp.zeros((2 * PER_GROUP, BLOCK), F32)
    for j in range(L_DEV // BLOCK):
        span = slice(j * BLOCK, (j + 1) * BLOCK)
        dt_j = dt[:, span]
        stacked = jnp.concatenate(three_pieces(rate[:, span]), axis=0).astype(BF16)
        sums = dot(stacked, upto)
        cs = sums[:HEADS] + sums[HEADS : 2 * HEADS] + sums[2 * HEADS :]
        row_ref[:, span] = cs - jnp.log2(dt_j)
        tail = three_pieces(jnp.exp2(cs[:, BLOCK - 1 :] - cs) * dt_j)
        grown = three_pieces(jnp.exp2(cs))
        sum_ref[span, :] = jnp.transpose(jnp.concatenate([cs, cs], axis=0))
        for g in range(GROUPS):
            heads = slice(g * PER_GROUP, (g + 1) * PER_GROUP)
            parts = [v[heads] for v in tail + grown] + [zero]
            col_ref[g, span, :] = jnp.transpose(jnp.concatenate(parts, axis=0)).astype(BF16)


def prep(step_raw, decay_rate):
    return pl.pallas_call(
        prep_kernel,
        out_shape=(
            jax.ShapeDtypeStruct((HEADS, L_DEV), F32),
            jax.ShapeDtypeStruct((L_DEV, 2 * HEADS), F32),
            jax.ShapeDtypeStruct((GROUPS, L_DEV, 128), BF16),
        ),
        cost_estimate=pl.CostEstimate(flops=10**9, bytes_accessed=2**21, transcendentals=0),
        compiler_params=pltpu.CompilerParams(vmem_limit_bytes=VMEM_LIMIT),
        name="prep",
    )(step_raw, decay_rate)


CONV_ROWS = 16


def taps(w_ref, bias_ref, lanes):
    w = w_ref[:, lanes].astype(F32) * 0.5
    return [w[k : k + 1] for k in range(4)], bias_ref[:, lanes].astype(F32) * 0.5


def silu_of(values, at, w, bias):
    half = bias + w[0] * values[at : at + CONV_ROWS, :]
    for k in range(1, 4):
        half = half + w[k] * values[at + k : at + k + CONV_ROWS, :]
    return half + half * jnp.tanh(half)


def conv_kernel(
    mask_ref, x_ref, b_ref, hx_ref, hb_ref, wx_ref, wb_ref, bx_ref, bb_ref, last_ref, col_ref,
    xo_ref, bo_ref, e0_ref, p_ref, xf, xs, tails, spread, regrown,
):
    within = mask_ref[0] % 4

    @pl.when(pl.program_id(0) == 0)
    def _():
        spread[...] = spread_matrix(TAIL)
        regrown[...] = spread_matrix(GROWN)

    def load(slot, ref, halo_ref, lanes):
        xf[slot, 5:8, :] = halo_ref[0, :, lanes].astype(F32)
        xf[slot, 8 : 8 + L_DEV, :] = ref[0, :, lanes].astype(F32)

    def widen(s):
        tails[s] = dot(col_ref[0], spread[:, s * OWN_CH : (s + 1) * OWN_CH])

    widen(0)
    ends = jnp.concatenate([col_ref[0, 240:256, :], col_ref[0, 496:512, :]], axis=0)
    decays = dot(ends, regrown[...])
    last = last_ref[0].astype(F32)[12:16]
    def emit(s):
        wide = slice(s * OWN_CH, (s + 1) * OWN_CH)
        first, second = decays[15:16, wide], decays[31:32, wide]
        e0 = dot(bt[0], xs[:BLOCK, wide])
        e1 = dot(bt[1], xs[BLOCK:, wide])
        e0_ref[0, :, wide] = e0.astype(BF16)
        slot = s ^ within
        p_ref[slot, :STATE, :] = (second * e0 + e1).astype(BF16)
        hi, mid, _ = three_pieces(first * second)
        at = CONV_AT[s]
        ends_of = [last[k : k + 1, at + 256 : at + 384] for k in range(4)]
        extra = [
            hi, mid, last[:, at : at + 256],
            jnp.concatenate(ends_of[:2], axis=1), jnp.concatenate(ends_of[2:], axis=1),
        ]
        p_ref[slot, STATE:, :] = jnp.concatenate(extra, axis=0).astype(BF16)

    for s in range(4):
        wide = slice(s * OWN_CH, (s + 1) * OWN_CH)
        pair = (2 * s, 2 * s + 1)
        both = []
        for k in pair:
            lanes = slice(k * 128, (k + 1) * 128)
            load(k, x_ref, hx_ref, lanes)
            both.append(taps(wx_ref, bx_ref, lanes))
        for r0 in range(0, L_DEV, CONV_ROWS):
            if r0 == 0 and s < 3:
                widen(s + 1)
            if r0 == 256 and s == 0:
                load(8, b_ref, hb_ref, slice(0, 128))
                w, bias = taps(wb_ref, bb_ref, slice(0, 128))
                for q in range(0, L_DEV, CONV_ROWS):
                    bo_ref[q : q + CONV_ROWS, :] = silu_of(xf.at[8], 5 + q, w, bias).astype(BF16)
                bt = [
                    jnp.transpose(bo_ref[j * BLOCK : (j + 1) * BLOCK, :].astype(F32)).astype(BF16) for j in range(2)
                ]
            if r0 == 0 and s > 0:
                emit(s - 1)
            rows = slice(r0, r0 + CONV_ROWS)
            parts = [silu_of(xf.at[k], 5 + r0, *tap) for k, tap in zip(pair, both)]
            value = jnp.concatenate(parts, axis=1)
            xo_ref[rows, wide] = value.astype(BF16)
            xs[rows, wide] = (value * tails[s, rows, :]).astype(BF16)
    emit(3)


CONV_AT = (0, 256, 640, 896)


def conv(rows, before, weight, bias, cols, mask):
    def whole(height, width, first):
        return pl.BlockSpec((1, height, width), lambda g, p: (0, 0, first + g))

    def flat(height, width, first):
        return pl.BlockSpec((height, width), lambda g, p: (0, first + g))

    return pl.pallas_call(
        conv_kernel,
        grid_spec=pltpu.PrefetchScalarGridSpec(
            num_scalar_prefetch=1,
            grid=(GROUPS,),
            in_specs=[
                whole(L_DEV, GROUP_CH, 0), whole(L_DEV, 128, 32),
                whole(3, GROUP_CH, 0), whole(3, 128, 32),
                flat(4, GROUP_CH, 0), flat(4, 128, 32),
                flat(1, GROUP_CH, 0), flat(1, 128, 32),
                pl.BlockSpec((1, 16, CH // GROUPS), lambda g, p: (0, L_DEV // 16 - 1, g)),
                pl.BlockSpec((1, L_DEV, 128), lambda g, p: (g, 0, 0)),
            ],
            out_specs=(
                flat(L_DEV, GROUP_CH, 0),
                flat(L_DEV, 128, 0),
                pl.BlockSpec((1, STATE, GROUP_CH), lambda g, p: (g, 0, 0)),
                pl.BlockSpec((4, SENT_ROWS, OWN_CH), lambda g, p: (g ^ (p[0] // 4), 0, 0)),
            ),
            scratch_shapes=[
                pltpu.VMEM((9, L_DEV + 8, 128), F32),
                pltpu.VMEM((L_DEV, GROUP_CH), BF16),
                pltpu.VMEM((4, L_DEV, OWN_CH), F32),
                pltpu.VMEM((128, GROUP_CH), BF16),
                pltpu.VMEM((128, GROUP_CH), BF16),
            ],
        ),
        out_shape=(
            jax.ShapeDtypeStruct((L_DEV, D_IN), BF16),
            jax.ShapeDtypeStruct((L_DEV, GROUPS * STATE), BF16),
            jax.ShapeDtypeStruct((GROUPS, STATE, GROUP_CH), BF16),
            jax.ShapeDtypeStruct((SHARDS, SENT_ROWS, OWN_CH), BF16),
        ),
        cost_estimate=pl.CostEstimate(flops=10 * 10**9, bytes_accessed=14 * 2**20, transcendentals=0),
        compiler_params=pltpu.CompilerParams(vmem_limit_bytes=VMEM_LIMIT),
        name="conv_state",
    )(mask, rows, rows, before, before, weight, weight, bias, bias, rows, cols)


def intra_kernel(
    x_ref, b_ref, c_ref, hc_ref, wc_ref, bc_ref, row_ref, col_ref, y_ref, co_ref, cf
):
    half = BLOCK // 2
    j = pl.program_id(1)
    sums = pltpu.roll(col_ref[...], (GROUPS - pl.program_id(0)) * PER_GROUP, 1)

    @pl.when(j == 0)
    def _():
        cf[5:8, :] = hc_ref[0].astype(F32)

    @pl.when(j == 1)
    def _():
        cf[0:8, :] = cf[BLOCK : BLOCK + 8, :]

    cf[8 : 8 + BLOCK, :] = c_ref[0].astype(F32)
    w, bias = taps(wc_ref, bc_ref, slice(0, 128))
    for r0 in range(0, BLOCK, CONV_ROWS):
        co_ref[r0 : r0 + CONV_ROWS, :] = silu_of(cf, 5 + r0, w, bias).astype(BF16)
    scores = lax.dot_general(
        co_ref[...], b_ref[...], (((1,), (1,)), ((), ())), preferred_element_type=F32
    )
    t = lax.broadcasted_iota(jnp.int32, (half, half), 0)
    u = lax.broadcasted_iota(jnp.int32, (half, half), 1)
    s00 = jnp.where(u <= t, scores[:half, :half], 0.0)
    s10 = scores[half:, :half]
    s11 = jnp.where(u <= t, scores[half:, half:], 0.0)
    low = lax.broadcasted_iota(jnp.int32, (BLOCK, 128), 1) < HEAD_DIM
    for pair in range(PER_GROUP // 2):
        lanes = slice(pair * 128, (pair + 1) * 128)
        x = x_ref[:, lanes]
        zero = jnp.zeros_like(x)
        xl, xh = jnp.where(low, x, zero), jnp.where(low, zero, x)
        top, bottom = [], []
        for h in (2 * pair, 2 * pair + 1):
            cs0 = jnp.broadcast_to(sums[:half, h : h + 1], (half, half))
            cs1 = jnp.broadcast_to(sums[half:, h : h + 1], (half, half))
            a0 = row_ref[h : h + 1, :half]
            a1 = row_ref[h : h + 1, half:]
            top.append((jnp.exp2(jnp.minimum(cs0 - a0, CAP)) * s00).astype(BF16))
            bottom.append((jnp.exp2(cs1 - a0) * s10).astype(BF16))
            bottom.append((jnp.exp2(jnp.minimum(cs1 - a1, CAP)) * s11).astype(BF16))
        above = dot(jnp.concatenate(top, axis=1), jnp.concatenate([xl[:half], xh[:half]], axis=0))
        below = dot(jnp.concatenate(bottom, axis=1), jnp.concatenate([xl, xh], axis=0))
        y_ref[:half, lanes] = above.astype(BF16)
        y_ref[half:, lanes] = below.astype(BF16)


def intra(x, b, rows, before, weight, bias, starts, sums):
    def at_c(g, j):
        return (0, D_IN // 128 + GROUPS + g)

    return pl.pallas_call(
        intra_kernel,
        grid=(GROUPS, L_DEV // BLOCK),
        in_specs=[
            pl.BlockSpec((BLOCK, GROUP_CH), lambda g, j: (j, g)),
            pl.BlockSpec((BLOCK, 128), lambda g, j: (j, g)),
            pl.BlockSpec((1, BLOCK, 128), lambda g, j: (0, j, at_c(g, j)[1])),
            pl.BlockSpec((1, 3, 128), lambda g, j: (0, 0, at_c(g, j)[1])),
            pl.BlockSpec((4, 128), at_c),
            pl.BlockSpec((1, 128), at_c),
            pl.BlockSpec((PER_GROUP, BLOCK), lambda g, j: (g, j)),
            pl.BlockSpec((BLOCK, 2 * HEADS), lambda g, j: (j, 0)),
        ],
        out_specs=(
            pl.BlockSpec((BLOCK, GROUP_CH), lambda g, j: (j, g)),
            pl.BlockSpec((BLOCK, 128), lambda g, j: (j, g)),
        ),
        out_shape=(
            jax.ShapeDtypeStruct((L_DEV, D_IN), BF16),
            jax.ShapeDtypeStruct((L_DEV, GROUPS * STATE), BF16),
        ),
        scratch_shapes=[pltpu.VMEM((BLOCK + 8, 128), F32)],
        cost_estimate=pl.CostEstimate(flops=12 * 10**9, bytes_accessed=12 * 2**20, transcendentals=0),
        compiler_params=pltpu.CompilerParams(vmem_limit_bytes=VMEM_LIMIT),
        name="intra",
    )(x, b, rows, before, weight, bias, starts, sums)


def scan_kernel(r_ref, p_ref, piece_ref):
    state = jnp.zeros((STATE, r_ref.shape[-1]), F32)
    for d in range(SHARDS):
        slot = d ^ FLIP
        p_ref[slot] = state.astype(BF16)
        extra = r_ref[slot, STATE:, :].astype(F32)
        state = (extra[0:1] + extra[1:2]) * state + r_ref[slot, :STATE, :].astype(F32)
    size = STATE // PIECES
    zero = jnp.zeros((PIECE_ROWS - size - 3, r_ref.shape[-1]), F32)
    for k in range(PIECES):
        rows = extra[2 + 2 * k : 4 + 2 * k]
        parts = [state[k * size : k * size + size], rows, extra[6 + k : 7 + k], zero]
        piece_ref[k * PIECE_ROWS : (k + 1) * PIECE_ROWS, :] = jnp.concatenate(parts, axis=0).astype(BF16)


def scan(got):
    return pl.pallas_call(
        scan_kernel,
        grid=(OWN_CH // 128,),
        in_specs=[pl.BlockSpec((SHARDS, SENT_ROWS, 128), lambda i: (0, 0, i))],
        out_specs=(
            pl.BlockSpec((SHARDS, STATE, 128), lambda i: (0, 0, i)),
            pl.BlockSpec((PIECES * PIECE_ROWS, 128), lambda i: (0, i)),
        ),
        out_shape=(
            jax.ShapeDtypeStruct((SHARDS, STATE, OWN_CH), BF16),
            jax.ShapeDtypeStruct((PIECES * PIECE_ROWS, OWN_CH), BF16),
        ),
        cost_estimate=pl.CostEstimate(flops=10**9, bytes_accessed=2**22, transcendentals=0),
        compiler_params=pltpu.CompilerParams(vmem_limit_bytes=VMEM_LIMIT),
        name="scan",
    )(got)


def pack_kernel(place_ref, prompt_ref, owner_ref, *refs):
    pieces, p_ref = refs[:-1], refs[-1]
    p_ref[...] = jnp.zeros_like(p_ref)
    for k in range(PIECES):
        p_ref[owner_ref[place_ref[0] ^ prompt_ref[0] ^ k] ^ FLIP] = pieces[k][...]


def pack(place, prompt, owner_slot, pieces):
    return pl.pallas_call(
        pack_kernel,
        in_specs=[SMEM] * 3 + [VMEM] * PIECES,
        out_shape=jax.ShapeDtypeStruct((SHARDS, PIECE_ROWS, OWN_CH), BF16),
        cost_estimate=pl.CostEstimate(flops=10**8, bytes_accessed=2**19, transcendentals=0),
        compiler_params=pltpu.CompilerParams(vmem_limit_bytes=VMEM_LIMIT),
        name="pack",
    )(place, prompt, owner_slot, *pieces)


def unpack_kernel(place_ref, prompt_ref, owner_ref, r_ref, ssm_ref, conv_ref):
    size = STATE // PIECES
    mine = 0
    for p in range(SHARDS):
        mine = jnp.where(owner_ref[p] == place_ref[0], p, mine)
    parts = [r_ref[mine ^ prompt_ref[0] ^ k ^ FLIP].astype(F32) for k in range(PIECES)]
    state = jnp.concatenate([part[:size] for part in parts], axis=0)
    ssm_ref[...] = jnp.transpose(state)
    rows = jnp.concatenate([part[size : size + 2] for part in parts], axis=0)
    ends = [part[size + 2 : size + 3, n * 128 : n * 128 + 128] for part in parts for n in range(2)]
    window = jnp.concatenate([rows, jnp.concatenate(ends, axis=0)], axis=1)
    moved = jnp.concatenate([window[:, 64:], window[:, :64]], axis=1)
    odd = prompt_ref[0] % 2 == 1
    conv_ref[...] = jnp.where(odd, moved, window)[:, : CH // SHARDS].astype(BF16)


def unpack(place, prompt, owner_slot, got):
    return pl.pallas_call(
        unpack_kernel,
        in_specs=[SMEM] * 3 + [VMEM],
        out_shape=(
            jax.ShapeDtypeStruct((OWN_CH, STATE), F32),
            jax.ShapeDtypeStruct((4, CH // SHARDS), BF16),
        ),
        cost_estimate=pl.CostEstimate(flops=10**8, bytes_accessed=2**19, transcendentals=0),
        compiler_params=pltpu.CompilerParams(vmem_limit_bytes=VMEM_LIMIT),
        name="unpack",
    )(place, prompt, owner_slot, got)


def out_kernel(mask_ref, y_ref, c_ref, col_ref, e0_ref, state_ref, gain_ref, o_ref, ys, spread):
    within = mask_ref[0] % 4

    @pl.when(pl.program_id(0) == 0)
    def _():
        spread[...] = spread_matrix(GROWN)

    decay = dot(col_ref[0, 240:256, :], spread[...])[15:16]
    for j in range(2):
        rows = slice(j * BLOCK, (j + 1) * BLOCK)
        c = c_ref[rows, :]
        grown = col_ref[0, rows, :]
        total = jnp.zeros((BLOCK, 128), F32)
        for s in range(4):
            lanes = slice(s * OWN_CH, (s + 1) * OWN_CH)
            state = state_ref[s ^ within]
            if j == 1:
                state = (decay[:, lanes] * state.astype(F32) + e0_ref[0, :, lanes].astype(F32)).astype(BF16)
            y = y_ref[rows, lanes].astype(F32) + dot(grown, spread[:, lanes]) * dot(c, state)
            ys[:, lanes] = y
            total = total + y[:, :128] * y[:, :128] + y[:, 128:] * y[:, 128:]
        mean = jnp.sum(total, axis=1, keepdims=True) * (1.0 / GROUP_CH)
        scale = lax.rsqrt(mean + NORM_EPS)
        o_ref[0, rows, :] = (ys[...] * scale * gain_ref[...]).astype(BF16)


def finish(y, c, cols, e0, states, gain, mask):
    return pl.pallas_call(
        out_kernel,
        grid_spec=pltpu.PrefetchScalarGridSpec(
            num_scalar_prefetch=1,
            grid=(GROUPS,),
            in_specs=[
                pl.BlockSpec((L_DEV, GROUP_CH), lambda g, m: (0, g)),
                pl.BlockSpec((L_DEV, 128), lambda g, m: (0, g)),
                pl.BlockSpec((1, L_DEV, 128), lambda g, m: (g, 0, 0)),
                pl.BlockSpec((1, STATE, GROUP_CH), lambda g, m: (g, 0, 0)),
                pl.BlockSpec((4, STATE, OWN_CH), lambda g, m: (g ^ (m[0] // 4), 0, 0)),
                pl.BlockSpec((1, GROUP_CH), lambda g, m: (0, g)),
            ],
            out_specs=pl.BlockSpec((1, L_DEV, GROUP_CH), lambda g, m: (0, 0, g)),
            scratch_shapes=[pltpu.VMEM((BLOCK, GROUP_CH), F32), pltpu.VMEM((128, GROUP_CH), BF16)],
        ),
        out_shape=jax.ShapeDtypeStruct((1, L_DEV, D_IN), BF16),
        cost_estimate=pl.CostEstimate(flops=8 * 10**9, bytes_accessed=12 * 2**20, transcendentals=0),
        compiler_params=pltpu.CompilerParams(vmem_limit_bytes=VMEM_LIMIT),
        name="finish",
    )(mask, y, c, cols, e0, states, gain)


def exchange(pieces):
    groups = [[(r ^ FLIP) * SHARDS + p for r in range(SHARDS)] for p in range(SHARDS)]
    return lax.all_to_all(
        pieces, ("seq", "grp"), split_axis=0, concat_axis=0, tiled=True, axis_index_groups=groups
    )


def body(conv_input, step_raw, decay_rate, conv_weight, conv_bias, norm_gain, owner_slot):
    place = lax.axis_index("seq").astype(jnp.int32)[None]
    prompt = lax.axis_index("grp").astype(jnp.int32)[None]
    route = [(d, d + 1) for d in range(SHARDS - 1)]
    before = lax.ppermute(conv_input[:, L_DEV - 3 :, :], "seq", route)
    starts, sums, cols = prep(step_raw, decay_rate[None, :])
    bias = conv_bias[None, :]
    x, b, e0, sent = conv(conv_input, before, conv_weight, bias, cols, prompt ^ FLIP)
    y, c = intra(x, b, conv_input, before, conv_weight, bias, starts, sums)
    got, y = lax.optimization_barrier((exchange(sent), y))
    states, final = scan(got)
    entering = exchange(states)
    turn = [
        (r * SHARDS + p, r * SHARDS + (r ^ p)) for r in range(SHARDS) for p in range(SHARDS)
    ]
    final = lax.ppermute(final, ("seq", "grp"), turn)
    kept, passed = final[:PIECE_ROWS], final[PIECE_ROWS:]
    pieces = [kept, lax.ppermute(passed, "seq", [(r, r ^ 1) for r in range(SHARDS)])]
    packed = pack(place, prompt, owner_slot, pieces)
    entering, packed = lax.optimization_barrier((entering, packed))
    arrived = exchange(packed)
    mixed = finish(y, c, cols, e0, entering, norm_gain[None, :], prompt ^ FLIP)
    ssm, rows = unpack(place, prompt, owner_slot, arrived)
    return mixed, ssm.reshape(1, 4, HEAD_DIM, STATE), jnp.transpose(rows)[None]


def solution(mesh):
    return jax.shard_map(
        body,
        mesh=mesh,
        in_specs=(P("grp", "seq", None), P("grp", None, "seq"), P(), P(), P(), P(), P()),
        out_specs=(P("grp", "seq", None), P("seq", "grp", None, None), P("seq", "grp", None)),
        check_vma=False,
    )
```
